256 devices in a mesh: row: 16 (over z, core), col: 16 (over x, y).
Axes of the slice: x: 4, y: 4, z: 8, core: 2. Of those that a mesh axis runs over, the one named last changes fastest.
Arguments:
- genotypes: int32 [4096, 16384], P(('row', 'col')), may hold values from 0 to 2, as said below
- snp_index: int32 [4096], P(('row', 'col')), may hold values from 0 to 16383, as said below
- freq_table: float32 [16384], replicated, as said below
- prior: float32 [16384, 16384], P('row', 'col'), as said below
- start_vectors: float32 [16384, 20], P('row'), may hold values from -6 to 6
Outputs:
- grm: float32 [16384, 16384], P('row', 'col')
- pcs: float32 [16384, 20], P('col')
- spectrum: float32 [3, 20], replicated
The draws below stay inside these ranges and needn't reach their ends.
Inputs may be any that keep to these rules, and one draw needn't show every extreme that they name: `genotypes`: genotype dosages 0, 1 or 2. `snp_index`: strictly increasing; entry j lies in 4 * j to 4 * j + 3. `freq_table`: frequencies are multiples of 1/1024 between 52/1024 and 512/1024. `prior`: exactly symmetric; diagonal between 1 and 2, off-diagonal entries small.
All inputs are finite; a program needn't handle non-finite values.
Results may differ from the reference program's by a relative error of at most 0.0075.
Values may be sent and summed in bfloat16 or wider, within the bound.
No kernel may reach another device: no remote copies, remote signals or barrier semaphores. Data moves between devices by JAX's collectives and lax.ppermute only.
A program may use at most 128 MiB of HBM per device.

```python
import jax
import jax.numpy as jnp
from jax import lax

S = 16384
M = 4096
STRIDE = 4
K = 20
ITERS = 3


def window_plan(key):
    offsets = jax.random.randint(jax.random.fold_in(key, 11), (M,), 0, STRIDE)
    positions = jnp.arange(M, dtype=jnp.int32) * STRIDE + offsets.astype(jnp.int32)
    numerators = jax.random.randint(jax.random.fold_in(key, 12), (M * STRIDE,), 52, 513)
    return (positions.astype(jnp.int32), numerators.astype(jnp.int32))


def draw_snp_index(key, part):
    positions, numerators = window_plan(key)
    return positions


def draw_freq_table(key, part):
    positions, numerators = window_plan(key)
    return numerators.astype(jnp.float32) / 1024.0


def draw_genotypes(key, part):
    positions, numerators = window_plan(key)
    chosen = jnp.take(numerators, positions)[:, None]
    first = jax.random.randint(jax.random.fold_in(key, 13), (M, S), 0, 1024)
    second = jax.random.randint(jax.random.fold_in(key, 14), (M, S), 0, 1024)
    return (first < chosen).astype(jnp.int32) + (second < chosen).astype(jnp.int32)


def draw_prior(key, part):
    noise = jax.random.normal(jax.random.fold_in(key, 21), (S, S), jnp.float32)
    offdiag = (noise + noise.T) * 0.002
    diagonal = jax.random.uniform(jax.random.fold_in(key, 22), (S,), jnp.float32, 1.0, 2.0)
    places = jnp.arange(S)
    return offdiag.at[places, places].set(diagonal)


def block_scale(rng, dims, shards, low, high):
    loudness, own = 1.0, jax.random.fold_in(rng, 6)
    for dim, blocks in shards:
        steps = jnp.exp(jax.random.uniform(jax.random.fold_in(own, dim), (blocks,), jnp.float32, low / len(shards), high / len(shards)))
        loudness = loudness * jnp.repeat(steps, dims[dim] // blocks).reshape([-1 if axis == dim else 1 for axis in range(len(dims))])
    return loudness


def bell_draw(key, dims, scale, reach, split=(), held_as=jnp.bfloat16):
    drawn = scale * jax.random.normal(key, dims, jnp.float32)
    if split:
        drawn = drawn * block_scale(key, dims, split, -0.22, 0.18)
    return jnp.clip(drawn, -reach, reach).astype(held_as)


def setup_inputs(seed: int = 0) -> dict:
    seeds = jax.random.split(jax.random.key(seed), 6)
    return {
        "genotypes": draw_genotypes(jax.random.fold_in(seeds[5], 71), 0),
        "snp_index": draw_snp_index(jax.random.fold_in(seeds[5], 71), 0),
        "freq_table": draw_freq_table(jax.random.fold_in(seeds[5], 71), 0),
        "prior": draw_prior(jax.random.fold_in(seeds[5], 71), 0),
        "start_vectors": bell_draw(seeds[4], (S, K), 1.0, 6.0, ((0, 16),), jnp.float32),
    }


def standardize(genotypes, allele_freq):
    doubled = 2.0 * allele_freq
    spread = jnp.sqrt(doubled * (1.0 - allele_freq))
    return (genotypes.astype(jnp.float32) - doubled[:, None]) / spread[:, None]

def orthonormal(factor, image):
    return lax.linalg.triangular_solve(factor, image, left_side=False, lower=True, transpose_a=True)

def reference(genotypes, snp_index, freq_table, prior, start_vectors):
    allele_freq = jnp.take(freq_table, snp_index.astype(jnp.int32))
    standard = standardize(genotypes, allele_freq).astype(jnp.bfloat16)
    widened = lax.optimization_barrier(standard).astype(jnp.float32)
    window = jnp.dot(widened.T, widened, precision=lax.Precision.HIGHEST)
    grm = prior + window / M
    vectors = start_vectors / jnp.sqrt(jnp.float32(S))
    diagonals = []
    for step in range(ITERS):
        image = jnp.dot(grm, vectors, precision=lax.Precision.HIGHEST)
        gram = jnp.dot(image.T, image, precision=lax.Precision.HIGHEST)
        factor = jnp.linalg.cholesky(gram)
        diagonals.append(jnp.diagonal(factor))
        vectors = orthonormal(factor, image)
    pcs = vectors * jnp.sqrt(jnp.float32(S))
    spectrum = jnp.stack(diagonals, axis=0)
    return (grm, pcs, spectrum)
```

```python
import jax
import jax.numpy as jnp
from jax import lax
from jax.sharding import Mesh
from jax.sharding import PartitionSpec as P

S = 16384
K = 20
ROW = ("z", "core")
COL = ("x", "y")
ALL = ("z", "core", "x", "y")
F32 = jnp.float32


def standardize(genotypes, allele_freq):
    doubled = 2.0 * allele_freq
    spread = jnp.sqrt(doubled * (1.0 - allele_freq))
    return (genotypes.astype(F32) - doubled[:, None]) / spread[:, None]


def bcast_sum(array, axis):
    length = lax.axis_size(axis)
    copies = jnp.broadcast_to(array[None], (length, *array.shape))
    return lax.all_to_all(copies, axis, 0, 0, tiled=True).sum(axis=0)


def swap_core(array):
    return lax.ppermute(array, "core", [(0, 1), (1, 0)])


def with_gram(wide, gram):
    width = wide.shape[1]
    flat = jnp.pad(gram.reshape(4, K * K // 4), ((0, 0), (0, width - K * K // 4)))
    return jnp.concatenate([wide, flat], axis=0)


def split_gram(packed):
    return packed[:K], packed[K:, : K * K // 4].reshape(K, K)


def row_sum(wide, gram=None):
    half = wide.shape[1] // 2
    first = lax.axis_index("core") == 0
    lo, hi = wide[:, :half], wide[:, half:]
    keep, give = jnp.where(first, lo, hi), jnp.where(first, hi, lo)
    if gram is not None:
        keep, give = with_gram(keep, gram), with_gram(give, gram)
    mine = bcast_sum(keep + swap_core(give), "z")
    if gram is not None:
        mine, gram = split_gram(mine)
    other = swap_core(mine)
    full = jnp.where(
        first,
        jnp.concatenate([mine, other], axis=1),
        jnp.concatenate([other, mine], axis=1),
    )
    return full if gram is None else (full, gram)


def col_sum(packed):
    return bcast_sum(bcast_sum(packed, "x"), "y")


def dot_t(a, b, dims):
    return lax.dot_general(a, b, (dims, ((), ())))


def forward(factor, wide):
    return lax.linalg.triangular_solve(factor, wide, left_side=True, lower=True)


def body(genotypes, snp_index, freq_table, prior, start_vectors):
    allele_freq = jnp.take(freq_table, snp_index)
    standard = standardize(genotypes, allele_freq).astype(jnp.bfloat16)
    row_count = lax.axis_size(ROW)
    col_count = lax.axis_size(COL)
    own_snps = genotypes.shape[0]
    total_snps = own_snps * row_count * col_count
    row_piece = lax.all_to_all(standard, ROW, split_axis=1, concat_axis=0, tiled=True)
    col_piece = lax.all_to_all(standard, COL, split_axis=1, concat_axis=0, tiled=True)
    col_piece = col_piece.reshape(col_count, 1, own_snps, col_piece.shape[1])
    col_panel = lax.all_gather(col_piece, ROW, axis=1, tiled=True)
    col_panel = col_panel.reshape(total_snps, col_panel.shape[3])
    window = lax.dot_general(
        lax.all_gather(row_piece, COL, axis=0, tiled=True),
        col_panel,
        (((0,), (0,)), ((), ())),
        preferred_element_type=F32,
    )
    grm = prior + window / total_snps
    start = start_vectors.T / jnp.sqrt(F32(S))
    image = row_sum(dot_t(start, grm, ((1,), (0,))))
    gram1 = dot_t(image, image, ((1,), (1,)))
    packed = with_gram(dot_t(image, grm, ((1,), (1,))), gram1)
    second, gram1 = split_gram(col_sum(packed))
    factor1 = jnp.linalg.cholesky(gram1)
    second = forward(factor1, second)
    third, gram2 = row_sum(
        dot_t(second, grm, ((1,), (0,))), dot_t(second, second, ((1,), (1,)))
    )
    gram3 = bcast_sum(dot_t(third, third, ((1,), (1,))), COL)
    factor2, factor3 = jnp.linalg.cholesky(jnp.stack([gram2, gram3]))
    vectors = forward(factor3, third)
    pcs = vectors.T * jnp.sqrt(F32(S))
    d1, d2, d3 = jnp.diagonal(factor1), jnp.diagonal(factor2), jnp.diagonal(factor3)
    return (grm, pcs, jnp.stack([d1, d2, d3 / d2], axis=0))


def solution(mesh):
    finer = Mesh(mesh.devices.reshape(8, 2, 4, 4), ALL)
    in_specs = (P(ALL, None), P(ALL), P(), P(ROW, COL), P(ROW, None))
    out_specs = (P(ROW, COL), P(COL, None), P())
    return jax.shard_map(body, mesh=finer, in_specs=in_specs, out_specs=out_specs, check_vma=False)
```

```python
import jax
import jax.numpy as jnp
from jax import lax
from jax.experimental import pallas as pl
from jax.experimental.pallas import tpu as pltpu
from jax.sharding import Mesh
from jax.sharding import PartitionSpec as P

S = 16384
M = 4096
K = 20
ROW = ("z", "core")
COL = ("x", "y")
ALL = ("z", "core", "x", "y")
SIZES = (8, 2, 4, 4)
F32 = jnp.float32
BF16 = jnp.bfloat16
VMEM = pl.BlockSpec(memory_space=pltpu.VMEM)
SMEM = pl.BlockSpec(memory_space=pltpu.SMEM)


def place(z, core, x, y):
    return ((z * 2 + core) * 4 + x) * 4 + y


def send(array, target):
    pairs = []
    for z in range(8):
        for core in range(2):
            for x in range(4):
                for y in range(4):
                    pairs.append((place(z, core, x, y), place(*target(z, core, x, y))))
    return lax.ppermute(array, ALL, pairs)


def swap_core(array):
    return send(array, lambda z, core, x, y: (z, 1 - core, x, y))


def ring_z(array):
    return send(array, lambda z, core, x, y: ((z + 1 - 2 * core) % 8, core, x, y))


def first_axis(array, step):
    def target(z, core, x, y):
        return (z, core, (x + step) % 4, y) if core == 0 else (z, core, x, (y + step) % 4)

    return send(array, target)


def second_axis(array, step):
    def target(z, core, x, y):
        return (z, core, (x + step) % 4, y) if core == 1 else (z, core, x, (y + step) % 4)

    return send(array, target)


def standardize_kernel(index, table, genotypes, out, rows):
    count = genotypes.shape[0]
    for j in range(count):
        rows[pl.ds(j, 1), :] = table[pl.ds(index[j] // 128, 1), :]
    lane = lax.broadcasted_iota(jnp.int32, (count, 128), 1)
    sub = lax.broadcasted_iota(jnp.int32, (count, 128), 0)
    want = jnp.zeros((count, 128), jnp.int32)
    for j in range(count):
        want = jnp.where(sub == j, index[j] % 128, want)
    freq = jnp.sum(jnp.where(lane == want, rows[...], 0.0), axis=1, keepdims=True)
    doubled = 2.0 * freq
    spread = jnp.sqrt(doubled * (1.0 - freq))
    value = (genotypes[...].astype(F32) - doubled) / spread
    out[0] = value.astype(BF16)


def standardize(genotypes, snp_index, freq_table):
    snps, samples = genotypes.shape
    return pl.pallas_call(
        standardize_kernel,
        grid_spec=pltpu.PrefetchScalarGridSpec(
            num_scalar_prefetch=1,
            grid=(16,),
            in_specs=[
                pl.BlockSpec((128, 128), lambda i, s: (0, 0)),
                pl.BlockSpec((snps, 1024), lambda i, s: (0, i)),
            ],
            out_specs=pl.BlockSpec((1, snps, 1024), lambda i, s: (i, 0, 0)),
            scratch_shapes=[pltpu.VMEM((snps, 128), F32)],
        ),
        out_shape=jax.ShapeDtypeStruct((16, snps, 1024), BF16),
        name="standardize",
    )(snp_index, freq_table.reshape(128, 128), genotypes)


def turn_kernel(order, piece, out, stage):
    for j in range(16):
        stage[16 * j : 16 * (j + 1), :] = piece[order[j]]
    out[...] = stage[...].T


def turn(order, piece):
    return pl.pallas_call(
        turn_kernel,
        in_specs=[SMEM, VMEM],
        out_specs=VMEM,
        out_shape=jax.ShapeDtypeStruct((1024, 256), BF16),
        scratch_shapes=[pltpu.VMEM((256, 1024), BF16)],
        name="turn",
    )(order, piece)


def make_tile_kernel(first, count):
    def kernel(index, *refs):
        columns, rows = refs[:16], refs[16 : 16 + count]
        base, out, stage = refs[16 + count :]
        for i in range(2 * count):
            which = index[2 * first + i]
            for j in range(16):
                stage[256 * i + 16 * j : 256 * i + 16 * (j + 1), :] = columns[j][which]

        def step(n, carry):
            at = pl.ds(pl.multiple_of(n * 256, 256), 256)
            total = jnp.zeros((1024, 256), F32)
            for i in range(count):
                total += jnp.dot(
                    rows[i][...], stage[512 * i : 512 * (i + 1), at], preferred_element_type=F32
                )
            out[:, at] = base[:, at] + total * (1.0 / M)
            return carry

        lax.fori_loop(0, 4, step, 0)

    return kernel


def tile(index, columns, rows, base, first, name, alias):
    count = len(rows)
    return pl.pallas_call(
        make_tile_kernel(first, count),
        in_specs=[SMEM] + [VMEM] * (16 + count + 1),
        out_specs=VMEM,
        out_shape=jax.ShapeDtypeStruct((1024, 1024), F32),
        scratch_shapes=[pltpu.VMEM((512 * count, 1024), BF16)],
        input_output_aliases={17 + count: 0} if alias else {},
        cost_estimate=pl.CostEstimate(
            flops=2 * 1024 * 1024 * 512 * count, bytes_accessed=2**20 * (8 + count), transcendentals=0
        ),
        name=name,
    )(index, *columns, *rows, base)


def bcast_sum(array, axis):
    length = lax.axis_size(axis)
    copies = jnp.broadcast_to(array[None], (length, *array.shape))
    return lax.all_to_all(copies, axis, 0, 0, tiled=True).sum(axis=0)


def with_gram(wide, gram):
    width = wide.shape[1]
    flat = jnp.pad(gram.reshape(4, K * K // 4), ((0, 0), (0, width - K * K // 4)))
    return jnp.concatenate([wide, flat], axis=0)


def split_gram(packed):
    return packed[:K], packed[K:, : K * K // 4].reshape(K, K)


def row_sum(wide, gram=None):
    half = wide.shape[1] // 2
    first = lax.axis_index("core") == 0
    lo, hi = wide[:, :half], wide[:, half:]
    keep, give = jnp.where(first, lo, hi), jnp.where(first, hi, lo)
    if gram is not None:
        keep, give = with_gram(keep, gram), with_gram(give, gram)
    mine = bcast_sum(keep + swap_core(give), "z")
    if gram is not None:
        mine, gram = split_gram(mine)
    other = swap_core(mine)
    full = jnp.where(
        first,
        jnp.concatenate([mine, other], axis=1),
        jnp.concatenate([other, mine], axis=1),
    )
    return full if gram is None else (full, gram)


def col_sum(packed):
    return bcast_sum(bcast_sum(packed, "x"), "y")


def dot_t(a, b, dims):
    return lax.dot_general(a, b, (dims, ((), ())))


def forward(factor, wide):
    return lax.linalg.triangular_solve(factor, wide, left_side=True, lower=True)


def body(genotypes, snp_index, freq_table, prior, start_vectors):
    z, core, x, y = (lax.axis_index(a) for a in ALL)
    sign = 1 - 2 * core
    steps = jnp.array([0, 0, -1, -1, -2, -2, -3, -3, -4, 1, 1, 2, 2, 3, 3, 4], jnp.int32)
    flips = jnp.array([0, 1, 0, 1, 0, 1, 0, 1, 0, 1, 0, 1, 0, 1, 0, 1], jnp.int32)
    order = ((z + sign * steps) % 8) * 2 + (core + flips) % 2
    along = jnp.array([0, -1, 1, 2] * 4, jnp.int32)
    across = jnp.array([0] * 4 + [-1] * 4 + [1] * 4 + [2] * 4, jnp.int32)
    index = ((x + jnp.where(core == 0, along, across)) % 4) * 4 + (
        y + jnp.where(core == 0, across, along)
    ) % 4

    standard = standardize(genotypes, snp_index, freq_table)
    own = lax.all_to_all(standard, COL, 0, 0, tiled=True)
    standard, own = lax.optimization_barrier((standard, own))
    a, b = own, swap_core(own)
    down, up = [a, b], []
    for j in range(1, 5):
        a = ring_z(a)
        down.append(a)
        up.append(swap_core(a))
        if j < 4:
            b = ring_z(b)
            down.append(b)
            up.append(swap_core(b))
    columns = down + up

    piece = lax.all_to_all(standard, ROW, 0, 0, tiled=True)
    piece = turn(order, piece)
    f, g = first_axis(piece, 1), first_axis(piece, -1)
    h, i = first_axis(f[:512], 1), first_axis(g[512:], -1)
    h0 = jnp.concatenate([piece, f], axis=1)
    h1 = jnp.concatenate([g, jnp.concatenate([h, i], axis=0)], axis=1)
    f0, f1 = second_axis(h0, 1), second_axis(h1, 1)
    g0, g1 = second_axis(h0, -1), second_axis(h1, -1)
    last0, last1 = second_axis(f0, 1), second_axis(g1, -1)
    partial = tile(index, columns, [h0, h1, f0, f1, g0, g1], prior, 0, "tile_a", False)
    grm = tile(index, columns, [last0, last1], partial, 6, "tile_b", True)

    start = start_vectors.T / jnp.sqrt(F32(S))
    image = row_sum(dot_t(start, grm, ((1,), (0,))))
    gram1 = dot_t(image, image, ((1,), (1,)))
    packed = with_gram(dot_t(image, grm, ((1,), (1,))), gram1)
    second, gram1 = split_gram(col_sum(packed))
    factor1 = jnp.linalg.cholesky(gram1)
    second = forward(factor1, second)
    third, gram2 = row_sum(
        dot_t(second, grm, ((1,), (0,))), dot_t(second, second, ((1,), (1,)))
    )
    gram3 = bcast_sum(dot_t(third, third, ((1,), (1,))), COL)
    factor2, factor3 = jnp.linalg.cholesky(jnp.stack([gram2, gram3]))
    vectors = forward(factor3, third)
    pcs = vectors.T * jnp.sqrt(F32(S))
    d1, d2, d3 = jnp.diagonal(factor1), jnp.diagonal(factor2), jnp.diagonal(factor3)
    return (grm, pcs, jnp.stack([d1, d2, d3 / d2], axis=0))


def solution(mesh):
    finer = Mesh(mesh.devices.reshape(SIZES), ALL)
    in_specs = (P(ALL, None), P(ALL), P(), P(ROW, COL), P(ROW, None))
    out_specs = (P(ROW, COL), P(COL, None), P())
    return jax.shard_map(body, mesh=finer, in_specs=in_specs, out_specs=out_specs, check_vma=False)
```

```python
import jax
import jax.numpy as jnp
from jax import lax
from jax.experimental import pallas as pl
from jax.experimental.pallas import tpu as pltpu
from jax.sharding import Mesh
from jax.sharding import PartitionSpec as P

S = 16384
M = 4096
K = 20
ROW = ("z", "core")
COL = ("x", "y")
ALL = ("z", "core", "x", "y")
SIZES = (8, 2, 4, 4)
F32 = jnp.float32
BF16 = jnp.bfloat16
VMEM = pl.BlockSpec(memory_space=pltpu.VMEM)
ANY = pl.BlockSpec(memory_space=pl.ANY)
SMEM = pl.BlockSpec(memory_space=pltpu.SMEM)


def place(z, core, x, y):
    return ((z * 2 + core) * 4 + x) * 4 + y


def send(array, target):
    pairs = []
    for z in range(8):
        for core in range(2):
            for x in range(4):
                for y in range(4):
                    pairs.append((place(z, core, x, y), place(*target(z, core, x, y))))
    return lax.ppermute(array, ALL, pairs)


def swap_core(array):
    return send(array, lambda z, core, x, y: (z, 1 - core, x, y))


def ring_z(array):
    return send(array, lambda z, core, x, y: ((z + 1 - 2 * core) % 8, core, x, y))


def first_axis(array, step):
    def target(z, core, x, y):
        return (z, core, (x + step) % 4, y) if core == 0 else (z, core, x, (y + step) % 4)

    return send(array, target)


def second_axis(array, step):
    def target(z, core, x, y):
        return (z, core, (x + step) % 4, y) if core == 1 else (z, core, x, (y + step) % 4)

    return send(array, target)


def standardize_kernel(index, table, genotypes, out, rows, doubled, spread):
    count = genotypes.shape[0]

    @pl.when(pl.program_id(0) == 0)
    def _():
        lane = lax.broadcasted_iota(jnp.int32, (count, 128), 1)
        sub = lax.broadcasted_iota(jnp.int32, (count, 128), 0)
        want = jnp.zeros((count, 128), jnp.int32)
        for j in range(count):
            rows[pl.ds(j, 1), :] = table[pl.ds(index[j] // 128, 1), :]
            want = jnp.where(sub == j, index[j] % 128, want)
        freq = jnp.sum(jnp.where(lane == want, rows[...], 0.0), axis=1, keepdims=True)
        doubled[...] = jnp.broadcast_to(2.0 * freq, (count, 128))
        spread[...] = jnp.broadcast_to(jnp.sqrt(2.0 * freq * (1.0 - freq)), (count, 128))

    blocks = out.shape[0]
    for i in range(blocks):
        value = genotypes[:, 1024 * i : 1024 * (i + 1)].astype(F32) - doubled[:, :1]
        out[i] = (value / spread[:, :1]).astype(BF16)


def standardize(genotypes, snp_index, freq_table):
    snps, samples = genotypes.shape
    return pl.pallas_call(
        standardize_kernel,
        grid_spec=pltpu.PrefetchScalarGridSpec(
            num_scalar_prefetch=1,
            grid=(4,),
            in_specs=[
                pl.BlockSpec((128, 128), lambda i, s: (0, 0)),
                pl.BlockSpec((snps, 4096), lambda i, s: (0, i)),
            ],
            out_specs=pl.BlockSpec((4, snps, 1024), lambda i, s: (i, 0, 0)),
            scratch_shapes=[pltpu.VMEM((snps, 128), F32)] * 3,
        ),
        out_shape=jax.ShapeDtypeStruct((16, snps, 1024), BF16),
        compiler_params=pltpu.CompilerParams(vmem_limit_bytes=8 * 2**20),
        name="standardize",
    )(snp_index, freq_table.reshape(128, 128), genotypes)


def turn_kernel(order, piece, out, stage):
    for j in range(16):
        stage[16 * j : 16 * (j + 1), :] = piece[order[j]]
    out[...] = stage[...].T


def turn(order, piece):
    return pl.pallas_call(
        turn_kernel,
        in_specs=[SMEM, VMEM],
        out_specs=VMEM,
        out_shape=jax.ShapeDtypeStruct((1024, 256), BF16),
        scratch_shapes=[pltpu.VMEM((256, 1024), BF16)],
        compiler_params=pltpu.CompilerParams(vmem_limit_bytes=8 * 2**20),
        name="turn",
    )(order, piece)


def make_tile_kernel(first, count, rounded):
    def kernel(index, *refs):
        columns, rows, base = refs[:16], refs[16 : 16 + count], refs[16 + count]
        outs, scratch = refs[17 + count : -7], refs[-7:]
        left, stage, total, base_sem, left_sem, stage_sem, out_sem = scratch
        from_base = pltpu.make_async_copy(base, total, base_sem)
        from_base.start()
        for i in range(count):
            pltpu.make_async_copy(rows[i], left.at[i], left_sem.at[i]).start()
            for t in range(2):
                which = index[2 * (first + i) + t]
                for j in range(16):
                    pltpu.make_async_copy(
                        columns[j].at[which],
                        stage.at[i, pl.ds(256 * t + 16 * j, 16)],
                        stage_sem.at[i],
                    ).start()
        from_base.wait()
        for i in range(count):
            pltpu.make_async_copy(rows[i], left.at[i], left_sem.at[i]).wait()
            pltpu.make_async_copy(stage.at[i], stage.at[i], stage_sem.at[i]).wait()

            def step(n, carry, i=i):
                at = pl.ds(pl.multiple_of(n * 256, 256), 256)
                product = jnp.dot(left[i], stage[i, :, at], preferred_element_type=F32)
                value = total[:, at] + product * (1.0 / M)
                total[:, at] = value
                if i == count - 1:
                    pltpu.make_async_copy(total.at[:, at], outs[0].at[:, at], out_sem.at[n]).start()
                    if rounded:
                        outs[1][:, at] = value.astype(BF16)
                return carry

            lax.fori_loop(0, 4, step, 0)
        for n in range(4):
            at = pl.ds(n * 256, 256)
            pltpu.make_async_copy(total.at[:, at], outs[0].at[:, at], out_sem.at[n]).wait()

    return kernel


def tile(index, columns, rows, base, first, name, rounded):
    count = len(rows)
    out_shape = [jax.ShapeDtypeStruct((1024, 1024), F32)]
    out_specs = [ANY]
    if rounded:
        out_shape.append(jax.ShapeDtypeStruct((1024, 1024), BF16))
        out_specs.append(VMEM)
    return pl.pallas_call(
        make_tile_kernel(first, count, rounded),
        in_specs=[SMEM] + [ANY] * (17 + count),
        out_specs=out_specs,
        out_shape=out_shape,
        scratch_shapes=[
            pltpu.VMEM((count, 1024, 512), BF16),
            pltpu.VMEM((count, 512, 1024), BF16),
            pltpu.VMEM((1024, 1024), F32),
            pltpu.SemaphoreType.DMA,
            pltpu.SemaphoreType.DMA((count,)),
            pltpu.SemaphoreType.DMA((count,)),
            pltpu.SemaphoreType.DMA((4,)),
        ],
        compiler_params=pltpu.CompilerParams(vmem_limit_bytes=(10 + 2 * count) * 2**20),
        cost_estimate=pl.CostEstimate(
            flops=2 * 1024 * 1024 * 512 * count, bytes_accessed=2**20 * (8 + 2 * count), transcendentals=0
        ),
        name=name,
    )(index, *columns, *rows, base)


def bcast_sum(array, axis):
    length = lax.axis_size(axis)
    copies = jnp.broadcast_to(array[None], (length, *array.shape))
    return lax.all_to_all(copies, axis, 0, 0, tiled=True).astype(F32).sum(axis=0)


def with_gram(wide, gram):
    width, quarter = wide.shape[1], K * K // 4
    high = lax.reduce_precision(gram, 8, 7)
    flat = jnp.concatenate([high.reshape(4, quarter), (gram - high).reshape(4, quarter)], axis=1)
    flat = jnp.pad(flat, ((0, 0), (0, width - 2 * quarter)))
    return jnp.concatenate([wide, flat], axis=0).astype(BF16)


def split_gram(packed):
    quarter = K * K // 4
    flat = packed[K:, :quarter] + packed[K:, quarter : 2 * quarter]
    return packed[:K], flat.reshape(K, K)


def row_sum(wide, gram=None):
    half = wide.shape[1] // 2
    first = lax.axis_index("core") == 0
    lo, hi = wide[:, :half], wide[:, half:]
    keep, give = jnp.where(first, lo, hi), jnp.where(first, hi, lo)
    mine = keep + swap_core(give)
    if gram is None:
        mine = bcast_sum(mine.astype(BF16), "z")
    else:
        mine, gram = split_gram(bcast_sum(with_gram(mine, gram), "z"))
        gram = gram + swap_core(gram)
    other = swap_core(mine)
    full = jnp.where(
        first,
        jnp.concatenate([mine, other], axis=1),
        jnp.concatenate([other, mine], axis=1),
    )
    return full if gram is None else (full, gram)


def dot_t(a, b, dims):
    return lax.dot_general(a, b, (dims, ((), ())), preferred_element_type=F32)


def eliminate(gram, wide=None):
    row = lax.broadcasted_iota(jnp.int32, (K, 1), 0)
    for j in range(K - 1):
        factor = jnp.where(row > j, gram[:, j : j + 1] / gram[j : j + 1, j : j + 1], 0.0)
        if wide is not None:
            wide = wide - factor * wide[j : j + 1, :]
        gram = gram - factor * gram[j : j + 1, :]
    eye = row == lax.broadcasted_iota(jnp.int32, (K, K), 1)
    pivots = jnp.where(eye, gram, 0.0)
    if wide is not None:
        wide = wide / jnp.sqrt(jnp.sum(pivots, axis=1, keepdims=True))
    return jnp.sqrt(jnp.sum(pivots, axis=0, keepdims=True)), wide


def solve_kernel(gram, wide, out, diagonal):
    diagonal[...], out[...] = eliminate(gram[...], wide[...])


def solve(gram, wide):
    return pl.pallas_call(
        solve_kernel,
        in_specs=[VMEM] * 2,
        out_specs=[VMEM] * 2,
        out_shape=[jax.ShapeDtypeStruct(wide.shape, F32), jax.ShapeDtypeStruct((1, K), F32)],
        compiler_params=pltpu.CompilerParams(vmem_limit_bytes=4 * 2**20),
        name="solve",
    )(gram, wide)


def last_kernel(first, gram2, gram3, wide, out, spectrum):
    second, _ = eliminate(gram2[...])
    third, vectors = eliminate(gram3[...], wide[...])
    out[...] = vectors * jnp.sqrt(F32(S))
    spectrum[0:1, :] = first[...]
    spectrum[1:2, :] = second
    spectrum[2:3, :] = third / second


def last(first, gram2, gram3, wide):
    return pl.pallas_call(
        last_kernel,
        in_specs=[VMEM] * 4,
        out_specs=[VMEM] * 2,
        out_shape=[jax.ShapeDtypeStruct(wide.shape, F32), jax.ShapeDtypeStruct((3, K), F32)],
        compiler_params=pltpu.CompilerParams(vmem_limit_bytes=4 * 2**20),
        name="last",
    )(first, gram2, gram3, wide)


def body(genotypes, snp_index, freq_table, prior, start_vectors):
    z, core, x, y = (lax.axis_index(a) for a in ALL)
    sign = 1 - 2 * core
    steps = jnp.array([0, 0, -1, -1, -2, -2, -3, -3, -4, 1, 1, 2, 2, 3, 3, 4], jnp.int32)
    flips = jnp.array([0, 1, 0, 1, 0, 1, 0, 1, 0, 1, 0, 1, 0, 1, 0, 1], jnp.int32)
    order = ((z + sign * steps) % 8) * 2 + (core + flips) % 2
    along = jnp.array([0, -1, 1, 2] * 4, jnp.int32)
    across = jnp.array([0] * 4 + [-1] * 4 + [1] * 4 + [2] * 4, jnp.int32)
    index = ((x + jnp.where(core == 0, along, across)) % 4) * 4 + (
        y + jnp.where(core == 0, across, along)
    ) % 4

    standard = standardize(genotypes, snp_index, freq_table)
    own = lax.all_to_all(standard, COL, 0, 0, tiled=True)
    standard, own = lax.optimization_barrier((standard, own))
    piece = lax.all_to_all(standard, ROW, 0, 0, tiled=True)
    own, piece = lax.optimization_barrier((own, piece))
    a, b = own, swap_core(own)
    down, up = [a, b], []
    for j in range(1, 5):
        a = ring_z(a)
        down.append(a)
        up.append(swap_core(a))
        if j < 4:
            b = ring_z(b)
            down.append(b)
            up.append(swap_core(b))
    columns = down + up

    piece = turn(order, piece)
    f, g = first_axis(piece, 1), first_axis(piece, -1)
    h, i = first_axis(f[:512], 1), first_axis(g[512:], -1)
    h0 = jnp.concatenate([piece, f], axis=1)
    h1 = jnp.concatenate([g, jnp.concatenate([h, i], axis=0)], axis=1)
    f0, f1 = second_axis(h0, 1), second_axis(h1, 1)
    g0, g1 = second_axis(h0, -1), second_axis(h1, -1)
    last0, last1 = second_axis(f0, 1), second_axis(g1, -1)
    (partial,) = tile(index, columns, [h0, h1, f0, f1, g0, g1], prior, 0, "tile_a", False)
    grm, rounded = tile(index, columns, [last0, last1], partial, 6, "tile_b", True)

    start = (start_vectors.T / jnp.sqrt(F32(S))).astype(BF16)
    image = row_sum(dot_t(start, rounded, ((1,), (0,))))
    gram1 = dot_t(image, image, ((1,), (1,)))
    packed = with_gram(dot_t(image.astype(BF16), rounded, ((1,), (1,))), gram1)
    second, gram1 = split_gram(bcast_sum(packed, COL))
    second, diagonal = solve(gram1, second)
    third, gram2 = row_sum(
        dot_t(second.astype(BF16), rounded, ((1,), (0,))), dot_t(second, second, ((1,), (1,)))
    )
    gram3 = bcast_sum(dot_t(third, third, ((1,), (1,))), COL)
    vectors, spectrum = last(diagonal, gram2, gram3, third)
    return (grm, vectors.T, spectrum)


def solution(mesh):
    finer = Mesh(mesh.devices.reshape(SIZES), ALL)
    in_specs = (P(ALL, None), P(ALL), P(), P(ROW, COL), P(ROW, None))
    out_specs = (P(ROW, COL), P(COL, None), P())
    return jax.shard_map(body, mesh=finer, in_specs=in_specs, out_specs=out_specs, check_vma=False)
```

```python
import jax
import jax.numpy as jnp
from jax import lax
from jax.experimental import pallas as pl
from jax.experimental.pallas import tpu as pltpu
from jax.sharding import Mesh
from jax.sharding import PartitionSpec as P


S = 16384
M = 4096
K = 20
ROW = ("z", "core")
COL = ("x", "y")
ALL = ("z", "core", "x", "y")
SIZES = (8, 2, 4, 4)
F32 = jnp.float32
BF16 = jnp.bfloat16
VMEM = pl.BlockSpec(memory_space=pltpu.VMEM)
ANY = pl.BlockSpec(memory_space=pl.ANY)
SMEM = pl.BlockSpec(memory_space=pltpu.SMEM)


def place(z, core, x, y):
    return ((z * 2 + core) * 4 + x) * 4 + y


def send(array, target):
    pairs = []
    for z in range(8):
        for core in range(2):
            for x in range(4):
                for y in range(4):
                    pairs.append((place(z, core, x, y), place(*target(z, core, x, y))))
    return lax.ppermute(array, ALL, pairs)


def swap_core(array):
    return send(array, lambda z, core, x, y: (z, 1 - core, x, y))


def ring_z(array):
    return send(array, lambda z, core, x, y: ((z + 1 - 2 * core) % 8, core, x, y))


def first_axis(array, step):
    def target(z, core, x, y):
        return (z, core, (x + step) % 4, y) if core == 0 else (z, core, x, (y + step) % 4)

    return send(array, target)


def second_axis(array, step):
    def target(z, core, x, y):
        return (z, core, (x + step) % 4, y) if core == 1 else (z, core, x, (y + step) % 4)

    return send(array, target)


def standardize_kernel(index, table, genotypes, out, rows, doubled, spread):
    count = genotypes.shape[0]

    @pl.when(pl.program_id(0) == 0)
    def _():
        lane = lax.broadcasted_iota(jnp.int32, (count, 128), 1)
        sub = lax.broadcasted_iota(jnp.int32, (count, 128), 0)
        want = jnp.zeros((count, 128), jnp.int32)
        for j in range(count):
            rows[pl.ds(j, 1), :] = table[pl.ds(index[j] // 128, 1), :]
            want = jnp.where(sub == j, index[j] % 128, want)
        freq = jnp.sum(jnp.where(lane == want, rows[...], 0.0), axis=1, keepdims=True)
        doubled[...] = jnp.broadcast_to(2.0 * freq, (count, 128))
        spread[...] = jnp.broadcast_to(jnp.sqrt(2.0 * freq * (1.0 - freq)), (count, 128))

    blocks = out.shape[0]
    for i in range(blocks):
        value = genotypes[:, 1024 * i : 1024 * (i + 1)].astype(F32) - doubled[:, :1]
        out[i] = (value / spread[:, :1]).astype(BF16)


def standardize(genotypes, snp_index, freq_table):
    snps, _ = genotypes.shape
    return pl.pallas_call(
        standardize_kernel,
        grid_spec=pltpu.PrefetchScalarGridSpec(
            num_scalar_prefetch=1,
            grid=(4,),
            in_specs=[
                pl.BlockSpec((128, 128), lambda i, s: (0, 0)),
                pl.BlockSpec((snps, 4096), lambda i, s: (0, i)),
            ],
            out_specs=pl.BlockSpec((4, snps, 1024), lambda i, s: (i, 0, 0)),
            scratch_shapes=[pltpu.VMEM((snps, 128), F32)] * 3,
        ),
        out_shape=jax.ShapeDtypeStruct((16, snps, 1024), BF16),
        compiler_params=pltpu.CompilerParams(vmem_limit_bytes=8 * 2**20),
        name="standardize",
    )(snp_index, freq_table.reshape(128, 128), genotypes)


def turn_kernel(order, piece, out, stage):
    for j in range(16):
        stage[16 * j : 16 * (j + 1), :] = piece[order[j]]
    out[...] = stage[...].T


def turn(order, piece):
    return pl.pallas_call(
        turn_kernel,
        in_specs=[SMEM, VMEM],
        out_specs=VMEM,
        out_shape=jax.ShapeDtypeStruct((1024, 256), BF16),
        scratch_shapes=[pltpu.VMEM((256, 1024), BF16)],
        compiler_params=pltpu.CompilerParams(vmem_limit_bytes=8 * 2**20),
        name="turn",
    )(order, piece)


def make_tile_kernel(first, count, rounded):
    def kernel(index, *refs):
        columns, rows, base = refs[:16], refs[16 : 16 + count], refs[16 + count]
        outs, scratch = refs[17 + count : -7], refs[-7:]
        if rounded:
            start, outs = outs[0], outs[1:]
        left, stage, total, base_sem, left_sem, stage_sem, out_sem = scratch
        from_base = pltpu.make_async_copy(base, total, base_sem)
        from_base.start()
        for i in range(count):
            pltpu.make_async_copy(rows[i], left.at[i], left_sem.at[i]).start()
            for t in range(2):
                which = index[2 * (first + i) + t]
                for j in range(16):
                    pltpu.make_async_copy(
                        columns[j].at[which],
                        stage.at[i, pl.ds(256 * t + 16 * j, 16)],
                        stage_sem.at[i],
                    ).start()
        from_base.wait()
        for i in range(count):
            pltpu.make_async_copy(rows[i], left.at[i], left_sem.at[i]).wait()
            pltpu.make_async_copy(stage.at[i], stage.at[i], stage_sem.at[i]).wait()

        def step(n, carry):
            at = pl.ds(pl.multiple_of(n * 256, 256), 256)
            product = jnp.zeros((1024, 256), F32)
            for i in range(count):
                product += jnp.dot(left[i], stage[i, :, at], preferred_element_type=F32)
            value = total[:, at] + product * (1.0 / M)
            total[:, at] = value
            pltpu.make_async_copy(total.at[:, at], outs[0].at[:, at], out_sem.at[n]).start()
            if rounded:
                outs[1][:, at] = value.astype(BF16)
                outs[2][:, at] = jnp.dot(
                    start[...], value.astype(BF16), preferred_element_type=F32
                )
            return carry

        lax.fori_loop(0, 4, step, 0)
        for n in range(4):
            at = pl.ds(n * 256, 256)
            pltpu.make_async_copy(total.at[:, at], outs[0].at[:, at], out_sem.at[n]).wait()

    return kernel


def tile(index, columns, rows, base, first, limit, start=None):
    count, rounded = len(rows), start is not None
    out_shape = [jax.ShapeDtypeStruct((1024, 1024), F32)]
    out_specs = [ANY]
    if rounded:
        out_shape += [jax.ShapeDtypeStruct((1024, 1024), BF16), jax.ShapeDtypeStruct((K, 1024), F32)]
        out_specs += [VMEM] * 2
    return pl.pallas_call(
        make_tile_kernel(first, count, rounded),
        in_specs=[SMEM] + [ANY] * (17 + count) + [VMEM] * rounded,
        out_specs=out_specs,
        out_shape=out_shape,
        scratch_shapes=[
            pltpu.VMEM((count, 1024, 512), BF16),
            pltpu.VMEM((count, 512, 1024), BF16),
            pltpu.VMEM((1024, 1024), F32),
            pltpu.SemaphoreType.DMA,
            pltpu.SemaphoreType.DMA((count,)),
            pltpu.SemaphoreType.DMA((count,)),
            pltpu.SemaphoreType.DMA((4,)),
        ],
        compiler_params=pltpu.CompilerParams(vmem_limit_bytes=limit * 2**20),
        cost_estimate=pl.CostEstimate(
            flops=2 * 1024 * 1024 * 512 * count, bytes_accessed=2**20 * (8 + 2 * count), transcendentals=0
        ),
    )(index, *columns, *rows, base, *([start] if rounded else []))


def bcast_sum(array, axis):
    length = lax.axis_size(axis)
    copies = jnp.broadcast_to(array[None], (length, *array.shape))
    return lax.all_to_all(copies, axis, 0, 0, tiled=True).astype(F32).sum(axis=0)


def with_gram(wide, gram):
    width, quarter = wide.shape[1], K * K // 4
    high = lax.reduce_precision(gram, 8, 7)
    flat = jnp.concatenate([high.reshape(4, quarter), (gram - high).reshape(4, quarter)], axis=1)
    flat = jnp.pad(flat, ((0, 0), (0, width - 2 * quarter)))
    return jnp.concatenate([wide, flat], axis=0).astype(BF16)


def split_gram(packed):
    quarter = K * K // 4
    flat = packed[K:, :quarter] + packed[K:, quarter : 2 * quarter]
    return packed[:K], flat.reshape(K, K)


def row_sum(wide, gram=None):
    half = wide.shape[1] // 2
    first = lax.axis_index("core") == 0
    lo, hi = wide[:, :half], wide[:, half:]
    keep, give = jnp.where(first, lo, hi), jnp.where(first, hi, lo)
    mine = keep + swap_core(give)
    if gram is None:
        mine = bcast_sum(mine.astype(BF16), "z")
    else:
        mine, gram = split_gram(bcast_sum(with_gram(mine, gram), "z"))
        gram = gram + swap_core(gram)
    other = swap_core(mine)
    full = jnp.where(
        first,
        jnp.concatenate([mine, other], axis=1),
        jnp.concatenate([other, mine], axis=1),
    )
    return full if gram is None else (full, gram)


def dot_t(a, b, dims):
    return lax.dot_general(a, b, (dims, ((), ())), preferred_element_type=F32)


def eliminate(gram, wide=None):
    row = lax.broadcasted_iota(jnp.int32, (K, 1), 0)
    for j in range(K - 1):
        factor = jnp.where(row > j, gram[:, j : j + 1] / gram[j : j + 1, j : j + 1], 0.0)
        if wide is not None:
            wide = wide - factor * wide[j : j + 1, :]
        gram = gram - factor * gram[j : j + 1, :]
    eye = row == lax.broadcasted_iota(jnp.int32, (K, K), 1)
    pivots = jnp.where(eye, gram, 0.0)
    if wide is not None:
        wide = wide / jnp.sqrt(jnp.sum(pivots, axis=1, keepdims=True))
    return jnp.sqrt(jnp.sum(pivots, axis=0, keepdims=True)), wide


def solve_kernel(gram, wide, out, diagonal):
    diagonal[...], out[...] = eliminate(gram[...], wide[...])


def solve(gram, wide):
    return pl.pallas_call(
        solve_kernel,
        in_specs=[VMEM] * 2,
        out_specs=[VMEM] * 2,
        out_shape=[jax.ShapeDtypeStruct(wide.shape, F32), jax.ShapeDtypeStruct((1, K), F32)],
        compiler_params=pltpu.CompilerParams(vmem_limit_bytes=4 * 2**20),
        name="solve",
    )(gram, wide)


def last_kernel(first, gram2, gram3, wide, out, spectrum):
    second, _ = eliminate(gram2[...])
    third, vectors = eliminate(gram3[...], wide[...])
    out[...] = vectors * jnp.sqrt(F32(S))
    spectrum[0:1, :] = first[...]
    spectrum[1:2, :] = second
    spectrum[2:3, :] = third / second


def last(first, gram2, gram3, wide):
    return pl.pallas_call(
        last_kernel,
        in_specs=[VMEM] * 4,
        out_specs=[VMEM] * 2,
        out_shape=[jax.ShapeDtypeStruct(wide.shape, F32), jax.ShapeDtypeStruct((3, K), F32)],
        compiler_params=pltpu.CompilerParams(vmem_limit_bytes=4 * 2**20),
        name="last",
    )(first, gram2, gram3, wide)


def body(genotypes, snp_index, freq_table, prior, start_vectors):
    z, core, x, y = (lax.axis_index(a) for a in ALL)
    sign = 1 - 2 * core
    steps = jnp.array([0, 0, -1, -1, -2, -2, -3, -3, -4, 1, 1, 2, 2, 3, 3, 4], jnp.int32)
    flips = jnp.array([0, 1, 0, 1, 0, 1, 0, 1, 0, 1, 0, 1, 0, 1, 0, 1], jnp.int32)
    order = ((z + sign * steps) % 8) * 2 + (core + flips) % 2
    along = jnp.array([0, -1, 1, 2] * 4, jnp.int32)
    across = jnp.array([0] * 4 + [-1] * 4 + [1] * 4 + [2] * 4, jnp.int32)
    index = ((x + jnp.where(core == 0, along, across)) % 4) * 4 + (
        y + jnp.where(core == 0, across, along)
    ) % 4

    standard = standardize(genotypes, snp_index, freq_table)
    own = lax.all_to_all(standard, COL, 0, 0, tiled=True)
    standard, own = lax.optimization_barrier((standard, own))
    a, b = own, swap_core(own)
    down, up = [a, b], []
    for j in range(1, 5):
        a = ring_z(a)
        down.append(a)
        up.append(swap_core(a))
        if j < 4:
            b = ring_z(b)
            down.append(b)
            up.append(swap_core(b))
    columns = down + up

    piece = lax.all_to_all(standard, ROW, 0, 0, tiled=True)
    piece = turn(order, piece)
    f = first_axis(piece, 1)
    g = first_axis(piece, -1)
    h = first_axis(f[:512], 1)
    i = first_axis(g[512:], -1)
    h0 = jnp.concatenate([piece, f], axis=1)
    h1 = jnp.concatenate([g, jnp.concatenate([h, i], axis=0)], axis=1)
    f0 = second_axis(h0, 1)
    g0 = second_axis(h0, -1)
    f1 = second_axis(h1, 1)
    g1 = second_axis(h1, -1)
    last0 = second_axis(f0, 1)
    last1 = second_axis(g1, -1)
    (partial,) = tile(index, columns, [h0, h1, f0, f1, g0, g1], prior, 0, 63)
    start = (start_vectors.T / jnp.sqrt(F32(S))).astype(BF16)
    grm, rounded, image = tile(index, columns, [last0, last1], partial, 6, 60, start)
    image = row_sum(image)
    gram1 = dot_t(image, image, ((1,), (1,)))
    packed = with_gram(dot_t(image.astype(BF16), rounded, ((1,), (1,))), gram1)
    second, gram1 = split_gram(bcast_sum(packed, COL))
    second, diagonal = solve(gram1, second)
    third, gram2 = row_sum(
        dot_t(second.astype(BF16), rounded, ((1,), (0,))), dot_t(second, second, ((1,), (1,)))
    )
    gram3 = bcast_sum(dot_t(third, third, ((1,), (1,))), COL)
    vectors, spectrum = last(diagonal, gram2, gram3, third)
    return (grm, vectors.T, spectrum)


def solution(mesh):
    finer = Mesh(mesh.devices.reshape(SIZES), ALL)
    in_specs = (P(ALL, None), P(ALL), P(), P(ROW, COL), P(ROW, None))
    out_specs = (P(ROW, COL), P(COL, None), P())
    return jax.shard_map(body, mesh=finer, in_specs=in_specs, out_specs=out_specs, check_vma=False)
```

```python
import jax
import jax.numpy as jnp
from jax import lax
from jax.experimental import pallas as pl
from jax.experimental.pallas import tpu as pltpu
from jax.sharding import Mesh
from jax.sharding import PartitionSpec as P


S = 16384
M = 4096
K = 20
ROW = ("z", "core")
COL = ("x", "y")
ALL = ("z", "core", "x", "y")
SIZES = (8, 2, 4, 4)
F32 = jnp.float32
BF16 = jnp.bfloat16
VMEM = pl.BlockSpec(memory_space=pltpu.VMEM)
ANY = pl.BlockSpec(memory_space=pl.ANY)
SMEM = pl.BlockSpec(memory_space=pltpu.SMEM)


def place(z, core, x, y):
    return ((z * 2 + core) * 4 + x) * 4 + y


def send(array, target):
    pairs = []
    for z in range(8):
        for core in range(2):
            for x in range(4):
                for y in range(4):
                    pairs.append((place(z, core, x, y), place(*target(z, core, x, y))))
    return lax.ppermute(array, ALL, pairs)


def swap_core(array):
    return send(array, lambda z, core, x, y: (z, 1 - core, x, y))


def ring_z(array):
    return send(array, lambda z, core, x, y: ((z + 1 - 2 * core) % 8, core, x, y))


def first_axis(array, step):
    def target(z, core, x, y):
        return (z, core, (x + step) % 4, y) if core == 0 else (z, core, x, (y + step) % 4)

    return send(array, target)


def second_axis(array, step):
    def target(z, core, x, y):
        return (z, core, (x + step) % 4, y) if core == 1 else (z, core, x, (y + step) % 4)

    return send(array, target)


def standardize_kernel(index, table, genotypes, out, rows, doubled, spread):
    count = genotypes.shape[0]

    @pl.when(pl.program_id(0) == 0)
    def _():
        lane = lax.broadcasted_iota(jnp.int32, (count, 128), 1)
        sub = lax.broadcasted_iota(jnp.int32, (count, 128), 0)
        want = jnp.zeros((count, 128), jnp.int32)
        for j in range(count):
            rows[pl.ds(j, 1), :] = table[pl.ds(index[j] // 128, 1), :]
            want = jnp.where(sub == j, index[j] % 128, want)
        freq = jnp.sum(jnp.where(lane == want, rows[...], 0.0), axis=1, keepdims=True)
        doubled[...] = jnp.broadcast_to(2.0 * freq, (count, 128))
        spread[...] = jnp.broadcast_to(jnp.sqrt(2.0 * freq * (1.0 - freq)), (count, 128))

    blocks = out.shape[0]
    for i in range(blocks):
        value = genotypes[:, 1024 * i : 1024 * (i + 1)].astype(F32) - doubled[:, :1]
        out[i] = (value / spread[:, :1]).astype(BF16)


def standardize(genotypes, snp_index, freq_table):
    snps, _ = genotypes.shape
    return pl.pallas_call(
        standardize_kernel,
        grid_spec=pltpu.PrefetchScalarGridSpec(
            num_scalar_prefetch=1,
            grid=(4,),
            in_specs=[
                pl.BlockSpec((128, 128), lambda i, s: (0, 0)),
                pl.BlockSpec((snps, 4096), lambda i, s: (0, i)),
            ],
            out_specs=pl.BlockSpec((4, snps, 1024), lambda i, s: (i, 0, 0)),
            scratch_shapes=[pltpu.VMEM((snps, 128), F32)] * 3,
        ),
        out_shape=jax.ShapeDtypeStruct((16, snps, 1024), BF16),
        compiler_params=pltpu.CompilerParams(vmem_limit_bytes=8 * 2**20),
        name="standardize",
    )(snp_index, freq_table.reshape(128, 128), genotypes)


def turn_kernel(order, piece, out, stage):
    for j in range(16):
        stage[16 * j : 16 * (j + 1), :] = piece[order[j]]
    out[...] = stage[...].T


def turn(order, piece):
    return pl.pallas_call(
        turn_kernel,
        in_specs=[SMEM, VMEM],
        out_specs=VMEM,
        out_shape=jax.ShapeDtypeStruct((1024, 256), BF16),
        scratch_shapes=[pltpu.VMEM((256, 1024), BF16)],
        compiler_params=pltpu.CompilerParams(vmem_limit_bytes=8 * 2**20),
        name="turn",
    )(order, piece)


def fetch_columns(index, columns, target, sem, first):
    for t in range(2):
        which = index[first + t]
        for j in range(16):
            pltpu.make_async_copy(
                columns[j].at[which], target.at[pl.ds(256 * t + 16 * j, 16)], sem
            ).start()


def tile_a_kernel(index, *refs):
    columns, rows, prior = refs[:16], refs[16:22], refs[22]
    total, ahead, left, stage, prior_sem, left_sem, stage_sem, ahead_sem = refs[23:]
    for i in range(2):
        pltpu.make_async_copy(rows[i], left.at[i], left_sem.at[i]).start()
        fetch_columns(index, columns, stage.at[i], stage_sem.at[i], 2 * i)
    from_prior = pltpu.make_async_copy(prior, total, prior_sem)
    from_prior.start()
    for i in range(2, 6):
        pltpu.make_async_copy(rows[i], left.at[i], left_sem.at[i]).start()
        fetch_columns(index, columns, stage.at[i], stage_sem.at[i], 2 * i)
    for i in range(2):
        fetch_columns(index, columns, ahead.at[pl.ds(512 * i, 512)], ahead_sem.at[i], 12 + 2 * i)
    for group in range(3):
        for i in (2 * group, 2 * group + 1):
            pltpu.make_async_copy(rows[i], left.at[i], left_sem.at[i]).wait()
            pltpu.make_async_copy(stage.at[i], stage.at[i], stage_sem.at[i]).wait()
        if group == 0:
            from_prior.wait()

        def step(n, carry, group=group):
            at = pl.ds(pl.multiple_of(n * 256, 256), 256)
            product = jnp.zeros((1024, 256), F32)
            for i in (2 * group, 2 * group + 1):
                product += jnp.dot(left[i], stage[i, :, at], preferred_element_type=F32)
            total[:, at] += product * (1.0 / M)
            return carry

        lax.fori_loop(0, 4, step, 0)
    for i in range(2):
        part = ahead.at[pl.ds(512 * i, 512)]
        pltpu.make_async_copy(part, part, ahead_sem.at[i]).wait()


def tile_a(index, columns, rows, prior):
    return pl.pallas_call(
        tile_a_kernel,
        in_specs=[SMEM] + [ANY] * 23,
        out_specs=[VMEM] * 2,
        out_shape=[jax.ShapeDtypeStruct((1024, 1024), F32), jax.ShapeDtypeStruct((1024, 1024), BF16)],
        scratch_shapes=[
            pltpu.VMEM((6, 1024, 512), BF16),
            pltpu.VMEM((6, 512, 1024), BF16),
            pltpu.SemaphoreType.DMA,
            pltpu.SemaphoreType.DMA((6,)),
            pltpu.SemaphoreType.DMA((6,)),
            pltpu.SemaphoreType.DMA((2,)),
        ],
        compiler_params=pltpu.CompilerParams(vmem_limit_bytes=32 * 2**20),
        cost_estimate=pl.CostEstimate(flops=6 * 2**30, bytes_accessed=18 * 2**20, transcendentals=0),
        name="tile_a",
    )(index, *columns, *rows, prior)


def tile_b_kernel(partial, ahead, row, start, out, rounded, image, total, out_sem):
    def step(n, carry):
        at = pl.ds(pl.multiple_of(n * 256, 256), 256)
        product = jnp.dot(row[...], ahead[:, at], preferred_element_type=F32)
        value = partial[:, at] + product * (1.0 / M)
        total[:, at] = value
        pltpu.make_async_copy(total.at[:, at], out.at[:, at], out_sem.at[n]).start()
        rounded[:, at] = value.astype(BF16)
        image[:, at] = jnp.dot(start[...], value.astype(BF16), preferred_element_type=F32)
        return carry

    lax.fori_loop(0, 4, step, 0)
    for n in range(4):
        at = pl.ds(n * 256, 256)
        pltpu.make_async_copy(total.at[:, at], out.at[:, at], out_sem.at[n]).wait()


def tile_b(partial, ahead, row, start):
    return pl.pallas_call(
        tile_b_kernel,
        in_specs=[VMEM] * 4,
        out_specs=[ANY, VMEM, VMEM],
        out_shape=[
            jax.ShapeDtypeStruct((1024, 1024), F32),
            jax.ShapeDtypeStruct((1024, 1024), BF16),
            jax.ShapeDtypeStruct((K, 1024), F32),
        ],
        scratch_shapes=[pltpu.VMEM((1024, 1024), F32), pltpu.SemaphoreType.DMA((4,))],
        compiler_params=pltpu.CompilerParams(vmem_limit_bytes=20 * 2**20),
        cost_estimate=pl.CostEstimate(flops=2 * 2**30, bytes_accessed=14 * 2**20, transcendentals=0),
        name="tile_b",
    )(partial, ahead, row, start)


def bcast_sum(array, axis):
    length = lax.axis_size(axis)
    copies = jnp.broadcast_to(array[None], (length, *array.shape))
    return lax.all_to_all(copies, axis, 0, 0, tiled=True).astype(F32).sum(axis=0)


def with_gram(wide, gram):
    width, quarter = wide.shape[1], K * K // 4
    high = lax.reduce_precision(gram, 8, 7)
    flat = jnp.concatenate([high.reshape(4, quarter), (gram - high).reshape(4, quarter)], axis=1)
    flat = jnp.pad(flat, ((0, 0), (0, width - 2 * quarter)))
    return jnp.concatenate([wide, flat], axis=0).astype(BF16)


def split_gram(packed):
    quarter = K * K // 4
    flat = packed[K:, :quarter] + packed[K:, quarter : 2 * quarter]
    return packed[:K], flat.reshape(K, K)


def row_sum(wide, gram=None):
    half = wide.shape[1] // 2
    first = lax.axis_index("core") == 0
    lo, hi = wide[:, :half], wide[:, half:]
    keep, give = jnp.where(first, lo, hi), jnp.where(first, hi, lo)
    mine = keep + swap_core(give)
    if gram is None:
        mine = bcast_sum(mine.astype(BF16), "z")
    else:
        mine, gram = split_gram(bcast_sum(with_gram(mine, gram), "z"))
        gram = gram + swap_core(gram)
    other = swap_core(mine)
    full = jnp.where(
        first,
        jnp.concatenate([mine, other], axis=1),
        jnp.concatenate([other, mine], axis=1),
    )
    return full if gram is None else (full, gram)


def dot_t(a, b, dims):
    return lax.dot_general(a, b, (dims, ((), ())), preferred_element_type=F32)


def eliminate(gram, wide=None):
    row = lax.broadcasted_iota(jnp.int32, (K, 1), 0)
    for j in range(K - 1):
        factor = jnp.where(row > j, gram[:, j : j + 1] / gram[j : j + 1, j : j + 1], 0.0)
        if wide is not None:
            wide = wide - factor * wide[j : j + 1, :]
        gram = gram - factor * gram[j : j + 1, :]
    eye = row == lax.broadcasted_iota(jnp.int32, (K, K), 1)
    pivots = jnp.where(eye, gram, 0.0)
    if wide is not None:
        wide = wide / jnp.sqrt(jnp.sum(pivots, axis=1, keepdims=True))
    return jnp.sqrt(jnp.sum(pivots, axis=0, keepdims=True)), wide


def solve_kernel(gram, wide, out, diagonal):
    diagonal[...], out[...] = eliminate(gram[...], wide[...])


def solve(gram, wide):
    return pl.pallas_call(
        solve_kernel,
        in_specs=[VMEM] * 2,
        out_specs=[VMEM] * 2,
        out_shape=[jax.ShapeDtypeStruct(wide.shape, F32), jax.ShapeDtypeStruct((1, K), F32)],
        compiler_params=pltpu.CompilerParams(vmem_limit_bytes=4 * 2**20),
        name="solve",
    )(gram, wide)


def last_kernel(first, gram2, gram3, wide, out, spectrum):
    second, _ = eliminate(gram2[...])
    third, vectors = eliminate(gram3[...], wide[...])
    out[...] = vectors * jnp.sqrt(F32(S))
    spectrum[0:1, :] = first[...]
    spectrum[1:2, :] = second
    spectrum[2:3, :] = third / second


def last(first, gram2, gram3, wide):
    return pl.pallas_call(
        last_kernel,
        in_specs=[VMEM] * 4,
        out_specs=[VMEM] * 2,
        out_shape=[jax.ShapeDtypeStruct(wide.shape, F32), jax.ShapeDtypeStruct((3, K), F32)],
        compiler_params=pltpu.CompilerParams(vmem_limit_bytes=4 * 2**20),
        name="last",
    )(first, gram2, gram3, wide)


def body(genotypes, snp_index, freq_table, prior, start_vectors):
    z, core, x, y = (lax.axis_index(a) for a in ALL)
    sign = 1 - 2 * core
    steps = jnp.array([0, 0, -1, -1, -2, -2, -3, -3, -4, 1, 1, 2, 2, 3, 3, 4], jnp.int32)
    flips = jnp.array([0, 1, 0, 1, 0, 1, 0, 1, 0, 1, 0, 1, 0, 1, 0, 1], jnp.int32)
    order = ((z + sign * steps) % 8) * 2 + (core + flips) % 2
    along = jnp.array([0, -1, 1, 2] * 4, jnp.int32)
    across = jnp.array([0] * 4 + [-1] * 4 + [1] * 4 + [2] * 4, jnp.int32)
    index = ((x + jnp.where(core == 0, along, across)) % 4) * 4 + (
        y + jnp.where(core == 0, across, along)
    ) % 4

    standard = standardize(genotypes, snp_index, freq_table)
    piece = lax.all_to_all(standard, ROW, 0, 0, tiled=True)
    standard, piece = lax.optimization_barrier((standard, piece))
    own = lax.all_to_all(standard, COL, 0, 0, tiled=True)
    a, b = own, swap_core(own)
    down, up = [a, b], []
    for j in range(1, 5):
        a = ring_z(a)
        down.append(a)
        up.append(swap_core(a))
        if j < 4:
            b = ring_z(b)
            down.append(b)
            up.append(swap_core(b))
    columns = down + up

    piece = turn(order, piece)
    f = first_axis(piece, 1)
    g = first_axis(piece, -1)
    h = first_axis(f[:512], 1)
    i = first_axis(g[512:], -1)
    h0 = jnp.concatenate([piece, f], axis=1)
    h1 = jnp.concatenate([g, jnp.concatenate([h, i], axis=0)], axis=1)
    f0 = second_axis(h0, 1)
    g0 = second_axis(h0, -1)
    f1 = second_axis(h1, 1)
    g1 = second_axis(h1, -1)
    last0 = second_axis(f0, 1)
    last1 = second_axis(g1, -1)
    partial, ahead = tile_a(index, columns, [h0, h1, f0, f1, g0, g1], prior)
    start = (start_vectors.T / jnp.sqrt(F32(S))).astype(BF16)
    ahead, last0, last1 = lax.optimization_barrier((ahead, last0, last1))
    grm, rounded, image = tile_b(partial, ahead, jnp.concatenate([last0, last1], axis=1), start)
    image = row_sum(image)
    gram1 = dot_t(image, image, ((1,), (1,)))
    packed = with_gram(dot_t(image.astype(BF16), rounded, ((1,), (1,))), gram1)
    second, gram1 = split_gram(bcast_sum(packed, COL))
    second, diagonal = solve(gram1, second)
    third, gram2 = row_sum(
        dot_t(second.astype(BF16), rounded, ((1,), (0,))), dot_t(second, second, ((1,), (1,)))
    )
    gram3 = bcast_sum(dot_t(third, third, ((1,), (1,))), COL)
    vectors, spectrum = last(diagonal, gram2, gram3, third)
    return (grm, vectors.T, spectrum)


def solution(mesh):
    finer = Mesh(mesh.devices.reshape(SIZES), ALL)
    in_specs = (P(ALL, None), P(ALL), P(), P(ROW, COL), P(ROW, None))
    out_specs = (P(ROW, COL), P(COL, None), P())
    return jax.shard_map(body, mesh=finer, in_specs=in_specs, out_specs=out_specs, check_vma=False)
```

```python
import jax
import jax.numpy as jnp
from jax import lax
from jax.experimental import pallas as pl
from jax.experimental.pallas import tpu as pltpu
from jax.sharding import Mesh
from jax.sharding import PartitionSpec as P


S = 16384
M = 4096
K = 20
ROW = ("z", "core")
COL = ("x", "y")
ALL = ("z", "core", "x", "y")
SIZES = (8, 2, 4, 4)
F32 = jnp.float32
BF16 = jnp.bfloat16
VMEM = pl.BlockSpec(memory_space=pltpu.VMEM)
ANY = pl.BlockSpec(memory_space=pl.ANY)
SMEM = pl.BlockSpec(memory_space=pltpu.SMEM)


def place(z, core, x, y):
    return ((z * 2 + core) * 4 + x) * 4 + y


def send(array, target):
    pairs = []
    for z in range(8):
        for core in range(2):
            for x in range(4):
                for y in range(4):
                    pairs.append((place(z, core, x, y), place(*target(z, core, x, y))))
    return lax.ppermute(array, ALL, pairs)


def swap_core(array):
    return send(array, lambda z, core, x, y: (z, 1 - core, x, y))


def ring_z(array):
    return send(array, lambda z, core, x, y: ((z + 1 - 2 * core) % 8, core, x, y))


def first_axis(array, step):
    def target(z, core, x, y):
        return (z, core, (x + step) % 4, y) if core == 0 else (z, core, x, (y + step) % 4)

    return send(array, target)


def second_axis(array, step):
    def target(z, core, x, y):
        return (z, core, (x + step) % 4, y) if core == 1 else (z, core, x, (y + step) % 4)

    return send(array, target)


def standardize_kernel(index, table, genotypes, out, rows, doubled, spread):
    count = genotypes.shape[0]

    @pl.when(pl.program_id(0) == 0)
    def _():
        lane = lax.broadcasted_iota(jnp.int32, (count, 128), 1)
        sub = lax.broadcasted_iota(jnp.int32, (count, 128), 0)
        want = jnp.zeros((count, 128), jnp.int32)
        for j in range(count):
            rows[pl.ds(j, 1), :] = table[pl.ds(index[j] // 128, 1), :]
            want = jnp.where(sub == j, index[j] % 128, want)
        freq = jnp.sum(jnp.where(lane == want, rows[...], 0.0), axis=1, keepdims=True)
        doubled[...] = jnp.broadcast_to(2.0 * freq, (count, 128))
        spread[...] = jnp.broadcast_to(jnp.sqrt(2.0 * freq * (1.0 - freq)), (count, 128))

    blocks = out.shape[0]
    for i in range(blocks):
        value = genotypes[:, 1024 * i : 1024 * (i + 1)].astype(F32) - doubled[:, :1]
        out[i] = (value / spread[:, :1]).astype(BF16)


def standardize(genotypes, snp_index, freq_table):
    snps, _ = genotypes.shape
    return pl.pallas_call(
        standardize_kernel,
        grid_spec=pltpu.PrefetchScalarGridSpec(
            num_scalar_prefetch=1,
            grid=(4,),
            in_specs=[
                pl.BlockSpec((128, 128), lambda i, s: (0, 0)),
                pl.BlockSpec((snps, 4096), lambda i, s: (0, i)),
            ],
            out_specs=pl.BlockSpec((4, snps, 1024), lambda i, s: (i, 0, 0)),
            scratch_shapes=[pltpu.VMEM((snps, 128), F32)] * 3,
        ),
        out_shape=jax.ShapeDtypeStruct((16, snps, 1024), BF16),
        compiler_params=pltpu.CompilerParams(vmem_limit_bytes=60 * 2**20),
        name="standardize",
    )(snp_index, freq_table.reshape(128, 128), genotypes)


def turn_kernel(order, piece, out, stage):
    for j in range(16):
        stage[16 * j : 16 * (j + 1), :] = piece[order[j]]
    out[...] = stage[...].T


def turn(order, piece):
    return pl.pallas_call(
        turn_kernel,
        in_specs=[SMEM, VMEM],
        out_specs=VMEM,
        out_shape=jax.ShapeDtypeStruct((1024, 256), BF16),
        scratch_shapes=[pltpu.VMEM((256, 1024), BF16)],
        compiler_params=pltpu.CompilerParams(vmem_limit_bytes=8 * 2**20),
        name="turn",
    )(order, piece)


def fetch_columns(index, columns, target, sem, first):
    for t in range(2):
        which = index[first + t]
        for j in range(16):
            pltpu.make_async_copy(
                columns[j].at[which], target.at[pl.ds(256 * t + 16 * j, 16)], sem
            ).start()


def tile_a_kernel(index, *refs):
    columns, rows, prior = refs[:16], refs[16:22], refs[22]
    total, ahead, left, stage, prior_sem, left_sem, stage_sem, ahead_sem = refs[23:]
    for i in range(2):
        pltpu.make_async_copy(rows[i], left.at[i], left_sem.at[i]).start()
        fetch_columns(index, columns, stage.at[i], stage_sem.at[i], 2 * i)
    from_prior = pltpu.make_async_copy(prior, total, prior_sem)
    from_prior.start()
    for i in range(2, 6):
        pltpu.make_async_copy(rows[i], left.at[i], left_sem.at[i]).start()
        fetch_columns(index, columns, stage.at[i], stage_sem.at[i], 2 * i)
    for i in range(2):
        fetch_columns(index, columns, ahead.at[pl.ds(512 * i, 512)], ahead_sem.at[i], 12 + 2 * i)
    for group in range(3):
        for i in (2 * group, 2 * group + 1):
            pltpu.make_async_copy(rows[i], left.at[i], left_sem.at[i]).wait()
            pltpu.make_async_copy(stage.at[i], stage.at[i], stage_sem.at[i]).wait()
        if group == 0:
            from_prior.wait()

        def step(n, carry, group=group):
            at = pl.ds(pl.multiple_of(n * 256, 256), 256)
            product = jnp.zeros((1024, 256), F32)
            for i in (2 * group, 2 * group + 1):
                product += jnp.dot(left[i], stage[i, :, at], preferred_element_type=F32)
            total[:, at] += product * (1.0 / M)
            return carry

        lax.fori_loop(0, 4, step, 0)
    for i in range(2):
        part = ahead.at[pl.ds(512 * i, 512)]
        pltpu.make_async_copy(part, part, ahead_sem.at[i]).wait()


def tile_a(index, columns, rows, prior):
    return pl.pallas_call(
        tile_a_kernel,
        in_specs=[SMEM] + [ANY] * 23,
        out_specs=[VMEM] * 2,
        out_shape=[jax.ShapeDtypeStruct((1024, 1024), F32), jax.ShapeDtypeStruct((1024, 1024), BF16)],
        scratch_shapes=[
            pltpu.VMEM((6, 1024, 512), BF16),
            pltpu.VMEM((6, 512, 1024), BF16),
            pltpu.SemaphoreType.DMA,
            pltpu.SemaphoreType.DMA((6,)),
            pltpu.SemaphoreType.DMA((6,)),
            pltpu.SemaphoreType.DMA((2,)),
        ],
        compiler_params=pltpu.CompilerParams(vmem_limit_bytes=32 * 2**20),
        cost_estimate=pl.CostEstimate(flops=6 * 2**30, bytes_accessed=18 * 2**20, transcendentals=0),
        name="tile_a",
    )(index, *columns, *rows, prior)


def tile_b_kernel(partial, ahead, row0, row1, start, out, rounded, image, total, out_sem):
    def step(n, carry):
        at = pl.ds(pl.multiple_of(n * 256, 256), 256)
        product = jnp.dot(row0[...], ahead[:512, at], preferred_element_type=F32)
        product += jnp.dot(row1[...], ahead[512:, at], preferred_element_type=F32)
        value = partial[:, at] + product * (1.0 / M)
        total[:, at] = value
        pltpu.make_async_copy(total.at[:, at], out.at[:, at], out_sem.at[n]).start()
        rounded[:, at] = value.astype(BF16)
        image[:, at] = jnp.dot(start[...], value.astype(BF16), preferred_element_type=F32)
        return carry

    lax.fori_loop(0, 4, step, 0)
    for n in range(4):
        at = pl.ds(n * 256, 256)
        pltpu.make_async_copy(total.at[:, at], out.at[:, at], out_sem.at[n]).wait()


def tile_b(partial, ahead, row0, row1, start):
    return pl.pallas_call(
        tile_b_kernel,
        in_specs=[VMEM] * 5,
        out_specs=[ANY, VMEM, VMEM],
        out_shape=[
            jax.ShapeDtypeStruct((1024, 1024), F32),
            jax.ShapeDtypeStruct((1024, 1024), BF16),
            jax.ShapeDtypeStruct((K, 1024), F32),
        ],
        scratch_shapes=[pltpu.VMEM((1024, 1024), F32), pltpu.SemaphoreType.DMA((4,))],
        compiler_params=pltpu.CompilerParams(vmem_limit_bytes=20 * 2**20),
        cost_estimate=pl.CostEstimate(flops=2 * 2**30, bytes_accessed=14 * 2**20, transcendentals=0),
        name="tile_b",
    )(partial, ahead, row0, row1, start)


def bcast_sum(array, axis):
    length = lax.axis_size(axis)
    copies = jnp.broadcast_to(array[None], (length, *array.shape))
    return lax.all_to_all(copies, axis, 0, 0, tiled=True).astype(F32).sum(axis=0)


def with_gram(wide, gram):
    width, quarter = wide.shape[1], K * K // 4
    high = lax.reduce_precision(gram, 8, 7)
    flat = jnp.concatenate([high.reshape(4, quarter), (gram - high).reshape(4, quarter)], axis=1)
    flat = jnp.pad(flat, ((0, 0), (0, width - 2 * quarter)))
    return jnp.concatenate([wide, flat], axis=0).astype(BF16)


def split_gram(packed):
    quarter = K * K // 4
    flat = packed[K:, :quarter] + packed[K:, quarter : 2 * quarter]
    return packed[:K], flat.reshape(K, K)


def row_sum(wide, gram=None):
    half = wide.shape[1] // 2
    first = lax.axis_index("core") == 0
    lo, hi = wide[:, :half], wide[:, half:]
    keep, give = jnp.where(first, lo, hi), jnp.where(first, hi, lo)
    mine = keep + swap_core(give)
    if gram is None:
        mine = bcast_sum(mine.astype(BF16), "z")
    else:
        mine, gram = split_gram(bcast_sum(with_gram(mine, gram), "z"))
        gram = gram + swap_core(gram)
    other = swap_core(mine)
    full = jnp.where(
        first,
        jnp.concatenate([mine, other], axis=1),
        jnp.concatenate([other, mine], axis=1),
    )
    return full if gram is None else (full, gram)


def dot_t(a, b, dims):
    return lax.dot_general(a, b, (dims, ((), ())), preferred_element_type=F32)


def eliminate(gram, wide=None):
    row = lax.broadcasted_iota(jnp.int32, (K, 1), 0)
    for j in range(K - 1):
        factor = jnp.where(row > j, gram[:, j : j + 1] / gram[j : j + 1, j : j + 1], 0.0)
        if wide is not None:
            wide = wide - factor * wide[j : j + 1, :]
        gram = gram - factor * gram[j : j + 1, :]
    eye = row == lax.broadcasted_iota(jnp.int32, (K, K), 1)
    pivots = jnp.where(eye, gram, 0.0)
    if wide is not None:
        wide = wide / jnp.sqrt(jnp.sum(pivots, axis=1, keepdims=True))
    return jnp.sqrt(jnp.sum(pivots, axis=0, keepdims=True)), wide


def solve_kernel(gram, wide, out, diagonal):
    diagonal[...], out[...] = eliminate(gram[...], wide[...])


def solve(gram, wide):
    return pl.pallas_call(
        solve_kernel,
        in_specs=[VMEM] * 2,
        out_specs=[VMEM] * 2,
        out_shape=[jax.ShapeDtypeStruct(wide.shape, F32), jax.ShapeDtypeStruct((1, K), F32)],
        compiler_params=pltpu.CompilerParams(vmem_limit_bytes=4 * 2**20),
        name="solve",
    )(gram, wide)


def last_kernel(first, gram2, gram3, wide, out, spectrum):
    second, _ = eliminate(gram2[...])
    third, vectors = eliminate(gram3[...], wide[...])
    out[...] = vectors * jnp.sqrt(F32(S))
    spectrum[0:1, :] = first[...]
    spectrum[1:2, :] = second
    spectrum[2:3, :] = third / second


def last(first, gram2, gram3, wide):
    return pl.pallas_call(
        last_kernel,
        in_specs=[VMEM] * 4,
        out_specs=[VMEM] * 2,
        out_shape=[jax.ShapeDtypeStruct(wide.shape, F32), jax.ShapeDtypeStruct((3, K), F32)],
        compiler_params=pltpu.CompilerParams(vmem_limit_bytes=4 * 2**20),
        name="last",
    )(first, gram2, gram3, wide)


def body(genotypes, snp_index, freq_table, prior, start_vectors):
    z, core, x, y = (lax.axis_index(a) for a in ALL)
    sign = 1 - 2 * core
    steps = jnp.array([0, 0, -1, -1, -2, -2, -3, -3, -4, 1, 1, 2, 2, 3, 3, 4], jnp.int32)
    flips = jnp.array([0, 1, 0, 1, 0, 1, 0, 1, 0, 1, 0, 1, 0, 1, 0, 1], jnp.int32)
    order = ((z + sign * steps) % 8) * 2 + (core + flips) % 2
    along = jnp.array([0, -1, 1, 2] * 4, jnp.int32)
    across = jnp.array([0] * 4 + [-1] * 4 + [1] * 4 + [2] * 4, jnp.int32)
    index = ((x + jnp.where(core == 0, along, across)) % 4) * 4 + (
        y + jnp.where(core == 0, across, along)
    ) % 4

    standard = standardize(genotypes, snp_index, freq_table)
    piece = lax.all_to_all(standard, ROW, 0, 0, tiled=True)
    standard, piece = lax.optimization_barrier((standard, piece))
    own = lax.all_to_all(standard, COL, 0, 0, tiled=True)
    a, b = own, swap_core(own)
    down, up = [a, b], []
    for j in range(1, 5):
        a = ring_z(a)
        down.append(a)
        up.append(swap_core(a))
        if j < 4:
            b = ring_z(b)
            down.append(b)
            up.append(swap_core(b))
    columns = down + up

    piece = turn(order, piece)
    f = first_axis(piece, 1)
    g = first_axis(piece, -1)
    h = first_axis(f[:512], 1)
    i = first_axis(g[512:], -1)
    h0 = jnp.concatenate([piece, f], axis=1)
    h1 = jnp.concatenate([g, jnp.concatenate([h, i], axis=0)], axis=1)
    f0 = second_axis(h0, 1)
    g0 = second_axis(h0, -1)
    f1 = second_axis(h1, 1)
    g1 = second_axis(h1, -1)
    last0 = second_axis(f0, 1)
    last1 = second_axis(g1, -1)
    partial, ahead = tile_a(index, columns, [h0, h1, f0, f1, g0, g1], prior)
    start = (start_vectors.T / jnp.sqrt(F32(S))).astype(BF16)
    ahead, last0, last1 = lax.optimization_barrier((ahead, last0, last1))
    grm, rounded, image = tile_b(partial, ahead, last0, last1, start)
    image = row_sum(image)
    gram1 = dot_t(image, image, ((1,), (1,)))
    packed = with_gram(dot_t(image.astype(BF16), rounded, ((1,), (1,))), gram1)
    packed = bcast_sum(packed, "x").astype(BF16)
    second, gram1 = split_gram(bcast_sum(packed, "y"))
    second, diagonal = solve(gram1, second)
    third, gram2 = row_sum(
        dot_t(second.astype(BF16), rounded, ((1,), (0,))), dot_t(second, second, ((1,), (1,)))
    )
    gram3 = jnp.pad(dot_t(third, third, ((1,), (1,))), ((0, 4), (0, 108)))
    gram3 = bcast_sum(gram3, COL)[:K, :K]
    vectors, spectrum = last(diagonal, gram2, gram3, third)
    return (grm, vectors.T, spectrum)


def solution(mesh):
    finer = Mesh(mesh.devices.reshape(SIZES), ALL)
    in_specs = (P(ALL, None), P(ALL), P(), P(ROW, COL), P(ROW, None))
    out_specs = (P(ROW, COL), P(COL, None), P())
    return jax.shard_map(body, mesh=finer, in_specs=in_specs, out_specs=out_specs, check_vma=False)
```

```python
import jax
import jax.numpy as jnp
from jax import lax
from jax.experimental import pallas as pl
from jax.experimental.pallas import tpu as pltpu
from jax.sharding import Mesh
from jax.sharding import PartitionSpec as P


S = 16384
M = 4096
K = 20
ROW = ("z", "core")
COL = ("x", "y")
ALL = ("z", "core", "x", "y")
SIZES = (8, 2, 4, 4)
F32 = jnp.float32
BF16 = jnp.bfloat16
VMEM = pl.BlockSpec(memory_space=pltpu.VMEM)
ANY = pl.BlockSpec(memory_space=pl.ANY)
SMEM = pl.BlockSpec(memory_space=pltpu.SMEM)


def place(z, core, x, y):
    return ((z * 2 + core) * 4 + x) * 4 + y


def send(array, target):
    pairs = []
    for z in range(8):
        for core in range(2):
            for x in range(4):
                for y in range(4):
                    pairs.append((place(z, core, x, y), place(*target(z, core, x, y))))
    return lax.ppermute(array, ALL, pairs)


def swap_core(array):
    return send(array, lambda z, core, x, y: (z, 1 - core, x, y))


def ring_z(array):
    return send(array, lambda z, core, x, y: ((z + 1 - 2 * core) % 8, core, x, y))


def first_axis(array, step):
    def target(z, core, x, y):
        return (z, core, (x + step) % 4, y) if core == 0 else (z, core, x, (y + step) % 4)

    return send(array, target)


def second_axis(array, step):
    def target(z, core, x, y):
        return (z, core, (x + step) % 4, y) if core == 1 else (z, core, x, (y + step) % 4)

    return send(array, target)


def standardize_kernel(index, table, genotypes, out, rows, doubled, spread):
    count = genotypes.shape[0]

    @pl.when(pl.program_id(0) == 0)
    def _():
        lane = lax.broadcasted_iota(jnp.int32, (count, 128), 1)
        sub = lax.broadcasted_iota(jnp.int32, (count, 128), 0)
        want = jnp.zeros((count, 128), jnp.int32)
        for j in range(count):
            rows[pl.ds(j, 1), :] = table[pl.ds(index[j] // 128, 1), :]
            want = jnp.where(sub == j, index[j] % 128, want)
        freq = jnp.sum(jnp.where(lane == want, rows[...], 0.0), axis=1, keepdims=True)
        doubled[...] = jnp.broadcast_to(2.0 * freq, (count, 128))
        spread[...] = jnp.broadcast_to(jnp.sqrt(2.0 * freq * (1.0 - freq)), (count, 128))

    blocks = out.shape[0]
    for i in range(blocks):
        value = genotypes[:, 1024 * i : 1024 * (i + 1)].astype(F32) - doubled[:, :1]
        out[i] = (value / spread[:, :1]).astype(BF16)


def standardize(genotypes, snp_index, freq_table):
    snps, _ = genotypes.shape
    return pl.pallas_call(
        standardize_kernel,
        grid_spec=pltpu.PrefetchScalarGridSpec(
            num_scalar_prefetch=1,
            grid=(4,),
            in_specs=[
                pl.BlockSpec((128, 128), lambda i, s: (0, 0)),
                pl.BlockSpec((snps, 4096), lambda i, s: (0, i)),
            ],
            out_specs=pl.BlockSpec((4, snps, 1024), lambda i, s: (i, 0, 0)),
            scratch_shapes=[pltpu.VMEM((snps, 128), F32)] * 3,
        ),
        out_shape=jax.ShapeDtypeStruct((16, snps, 1024), BF16),
        compiler_params=pltpu.CompilerParams(vmem_limit_bytes=60 * 2**20),
        name="standardize",
    )(snp_index, freq_table.reshape(128, 128), genotypes)


def turn_kernel(order, piece, out, stage):
    for j in range(16):
        stage[16 * j : 16 * (j + 1), :] = piece[order[j]]
    out[...] = stage[...].T


def turn(order, piece):
    return pl.pallas_call(
        turn_kernel,
        in_specs=[SMEM, VMEM],
        out_specs=VMEM,
        out_shape=jax.ShapeDtypeStruct((1024, 256), BF16),
        scratch_shapes=[pltpu.VMEM((256, 1024), BF16)],
        compiler_params=pltpu.CompilerParams(vmem_limit_bytes=8 * 2**20),
        name="turn",
    )(order, piece)


def fetch_columns(index, columns, target, sem, first):
    for t in range(2):
        which = index[first + t]
        for j in range(16):
            pltpu.make_async_copy(
                columns[j].at[which], target.at[pl.ds(256 * t + 16 * j, 16)], sem
            ).start()


def tile_a_kernel(index, *refs):
    columns, rows, prior, spread = refs[:16], refs[16:22], refs[22], refs[23]
    total, ahead, image, left, stage, prior_sem, left_sem, stage_sem, ahead_sem = refs[24:]

    def fetch_row(i):
        return pltpu.make_async_copy(rows[i], left.at[i, pl.ds(0, 1024)], left_sem.at[i])

    for i in range(2):
        fetch_row(i).start()
        fetch_columns(index, columns, stage.at[i], stage_sem.at[i], 2 * i)
    from_prior = pltpu.make_async_copy(prior, total, prior_sem)
    from_prior.start()
    for i in range(2, 6):
        fetch_row(i).start()
        fetch_columns(index, columns, stage.at[i], stage_sem.at[i], 2 * i)
    for i in range(2):
        fetch_columns(index, columns, ahead.at[pl.ds(512 * i, 512)], ahead_sem.at[i], 12 + 2 * i)
    for i in range(6):
        for t in range(2):
            left[i, 1024:1056, 256 * t : 256 * (t + 1)] = spread[index[2 * i + t]]
    for group in range(3):
        for i in (2 * group, 2 * group + 1):
            fetch_row(i).wait()
            pltpu.make_async_copy(stage.at[i], stage.at[i], stage_sem.at[i]).wait()
        if group == 0:
            from_prior.wait()

        def step(n, carry, group=group):
            at = pl.ds(pl.multiple_of(n * 256, 256), 256)
            product = jnp.zeros((1056, 256), F32)
            for i in (2 * group, 2 * group + 1):
                product += jnp.dot(left[i], stage[i, :, at], preferred_element_type=F32)
            total[:, at] += product[:1024] * (1.0 / M)
            if group == 0:
                image[:, at] = product[1024:]
            else:
                image[:, at] += product[1024:]
            return carry

        lax.fori_loop(0, 4, step, 0)
    for i in range(2):
        part = ahead.at[pl.ds(512 * i, 512)]
        pltpu.make_async_copy(part, part, ahead_sem.at[i]).wait()


def tile_a(index, columns, rows, prior, spread):
    return pl.pallas_call(
        tile_a_kernel,
        in_specs=[SMEM] + [ANY] * 23 + [VMEM],
        out_specs=[VMEM] * 3,
        out_shape=[
            jax.ShapeDtypeStruct((1024, 1024), F32),
            jax.ShapeDtypeStruct((1024, 1024), BF16),
            jax.ShapeDtypeStruct((32, 1024), F32),
        ],
        scratch_shapes=[
            pltpu.VMEM((6, 1056, 512), BF16),
            pltpu.VMEM((6, 512, 1024), BF16),
            pltpu.SemaphoreType.DMA,
            pltpu.SemaphoreType.DMA((6,)),
            pltpu.SemaphoreType.DMA((6,)),
            pltpu.SemaphoreType.DMA((2,)),
        ],
        compiler_params=pltpu.CompilerParams(vmem_limit_bytes=32 * 2**20),
        cost_estimate=pl.CostEstimate(flops=6 * 2**30, bytes_accessed=18 * 2**20, transcendentals=0),
        name="tile_a",
    )(index, *columns, *rows, prior, spread)


def tile_b_kernel(
    index, partial, ahead, row0, row1, spread, so_far, first, out, rounded, image, total, left, out_sem
):
    for t in range(4):
        left[:, 256 * t : 256 * (t + 1)] = spread[index[12 + t]]

    def step(n, carry):
        at = pl.ds(pl.multiple_of(n * 256, 256), 256)
        product = jnp.dot(row0[...], ahead[:512, at], preferred_element_type=F32)
        product += jnp.dot(row1[...], ahead[512:, at], preferred_element_type=F32)
        value = partial[:, at] + product * (1.0 / M)
        total[:, at] = value
        pltpu.make_async_copy(total.at[:, at], out.at[:, at], out_sem.at[n]).start()
        rounded[:, at] = value.astype(BF16)
        rest = so_far[:, at] + jnp.dot(left[...], ahead[:, at], preferred_element_type=F32)
        image[:, at] = first[:, at] + rest[:K] * (1.0 / M)
        return carry

    lax.fori_loop(0, 4, step, 0)
    for n in range(4):
        at = pl.ds(n * 256, 256)
        pltpu.make_async_copy(total.at[:, at], out.at[:, at], out_sem.at[n]).wait()


def tile_b(index, partial, ahead, row0, row1, spread, so_far, first):
    return pl.pallas_call(
        tile_b_kernel,
        in_specs=[SMEM] + [VMEM] * 7,
        out_specs=[ANY, VMEM, VMEM],
        out_shape=[
            jax.ShapeDtypeStruct((1024, 1024), F32),
            jax.ShapeDtypeStruct((1024, 1024), BF16),
            jax.ShapeDtypeStruct((K, 1024), F32),
        ],
        scratch_shapes=[
            pltpu.VMEM((1024, 1024), F32),
            pltpu.VMEM((32, 1024), BF16),
            pltpu.SemaphoreType.DMA((4,)),
        ],
        compiler_params=pltpu.CompilerParams(vmem_limit_bytes=20 * 2**20),
        cost_estimate=pl.CostEstimate(flops=2 * 2**30, bytes_accessed=14 * 2**20, transcendentals=0),
        name="tile_b",
    )(index, partial, ahead, row0, row1, spread, so_far, first)


def bcast_sum(array, axis):
    length = lax.axis_size(axis)
    copies = jnp.broadcast_to(array[None], (length, *array.shape))
    return lax.all_to_all(copies, axis, 0, 0, tiled=True).astype(F32).sum(axis=0)


def with_gram(wide, gram):
    width, quarter = wide.shape[1], K * K // 4
    high = lax.reduce_precision(gram, 8, 7)
    flat = jnp.concatenate([high.reshape(4, quarter), (gram - high).reshape(4, quarter)], axis=1)
    flat = jnp.pad(flat, ((0, 0), (0, width - 2 * quarter)))
    return jnp.concatenate([wide, flat], axis=0).astype(BF16)


def split_gram(packed):
    quarter = K * K // 4
    flat = packed[K:, :quarter] + packed[K:, quarter : 2 * quarter]
    return packed[:K], flat.reshape(K, K)


def row_sum(wide, gram=None):
    half = wide.shape[1] // 2
    first = lax.axis_index("core") == 0
    lo, hi = wide[:, :half], wide[:, half:]
    keep, give = jnp.where(first, lo, hi), jnp.where(first, hi, lo)
    mine = keep + swap_core(give)
    if gram is None:
        mine = bcast_sum(mine.astype(BF16), "z")
    else:
        mine, gram = split_gram(bcast_sum(with_gram(mine, gram), "z"))
        gram = gram + swap_core(gram)
    other = swap_core(mine)
    full = jnp.where(
        first,
        jnp.concatenate([mine, other], axis=1),
        jnp.concatenate([other, mine], axis=1),
    )
    return full if gram is None else (full, gram)


def dot_t(a, b, dims):
    return lax.dot_general(a, b, (dims, ((), ())), preferred_element_type=F32)


def eliminate(gram, wide=None):
    row = lax.broadcasted_iota(jnp.int32, (K, 1), 0)
    for j in range(K - 1):
        factor = jnp.where(row > j, gram[:, j : j + 1] / gram[j : j + 1, j : j + 1], 0.0)
        if wide is not None:
            wide = wide - factor * wide[j : j + 1, :]
        gram = gram - factor * gram[j : j + 1, :]
    eye = row == lax.broadcasted_iota(jnp.int32, (K, K), 1)
    pivots = jnp.where(eye, gram, 0.0)
    if wide is not None:
        wide = wide / jnp.sqrt(jnp.sum(pivots, axis=1, keepdims=True))
    return jnp.sqrt(jnp.sum(pivots, axis=0, keepdims=True)), wide


def solve_kernel(gram, wide, out, diagonal):
    diagonal[...], out[...] = eliminate(gram[...], wide[...])


def solve(gram, wide):
    return pl.pallas_call(
        solve_kernel,
        in_specs=[VMEM] * 2,
        out_specs=[VMEM] * 2,
        out_shape=[jax.ShapeDtypeStruct(wide.shape, F32), jax.ShapeDtypeStruct((1, K), F32)],
        compiler_params=pltpu.CompilerParams(vmem_limit_bytes=4 * 2**20),
        name="solve",
    )(gram, wide)


def last_kernel(first, gram2, gram3, wide, out, spectrum):
    second, _ = eliminate(gram2[...])
    third, vectors = eliminate(gram3[...], wide[...])
    out[...] = vectors * jnp.sqrt(F32(S))
    spectrum[0:1, :] = first[...]
    spectrum[1:2, :] = second
    spectrum[2:3, :] = third / second


def last(first, gram2, gram3, wide):
    return pl.pallas_call(
        last_kernel,
        in_specs=[VMEM] * 4,
        out_specs=[VMEM] * 2,
        out_shape=[jax.ShapeDtypeStruct(wide.shape, F32), jax.ShapeDtypeStruct((3, K), F32)],
        compiler_params=pltpu.CompilerParams(vmem_limit_bytes=4 * 2**20),
        name="last",
    )(first, gram2, gram3, wide)


def body(genotypes, snp_index, freq_table, prior, start_vectors):
    z, core, x, y = (lax.axis_index(a) for a in ALL)
    sign = 1 - 2 * core
    steps = jnp.array([0, 0, -1, -1, -2, -2, -3, -3, -4, 1, 1, 2, 2, 3, 3, 4], jnp.int32)
    flips = jnp.array([0, 1, 0, 1, 0, 1, 0, 1, 0, 1, 0, 1, 0, 1, 0, 1], jnp.int32)
    order = ((z + sign * steps) % 8) * 2 + (core + flips) % 2
    along = jnp.array([0, -1, 1, 2] * 4, jnp.int32)
    across = jnp.array([0] * 4 + [-1] * 4 + [1] * 4 + [2] * 4, jnp.int32)
    index = ((x + jnp.where(core == 0, along, across)) % 4) * 4 + (
        y + jnp.where(core == 0, across, along)
    ) % 4

    standard = standardize(genotypes, snp_index, freq_table)
    piece = lax.all_to_all(standard, ROW, 0, 0, tiled=True)
    standard, piece = lax.optimization_barrier((standard, piece))
    own = lax.all_to_all(standard, COL, 0, 0, tiled=True)
    a, b = own, swap_core(own)
    down, up = [a, b], []
    for j in range(1, 5):
        a = ring_z(a)
        down.append(a)
        up.append(swap_core(a))
        if j < 4:
            b = ring_z(b)
            down.append(b)
            up.append(swap_core(b))
    columns = down + up

    start = (start_vectors.T / jnp.sqrt(F32(S))).astype(BF16)
    parts = [
        dot_t(start, prior.astype(BF16), ((1,), (0,))),
        dot_t(start, piece.reshape(256, 1024), ((1,), (1,))),
    ]
    early = row_sum(jnp.concatenate(parts, axis=1))
    spread = jnp.pad(early[:, 1024:], ((0, 32 - K), (0, 0))).astype(BF16)
    spread = lax.all_to_all(jnp.broadcast_to(spread[None], (16, 32, 256)), COL, 0, 0, tiled=True)
    at = jnp.arange(256, dtype=jnp.int32)
    moved = jnp.broadcast_to(order[:, None], (16, 16)).reshape(1, 256) * 16 + at[None] % 16
    moved = (at[:, None] == moved).astype(BF16)
    spread = dot_t(spread.reshape(512, 256), moved, ((1,), (0,))).astype(BF16)
    spread = spread.reshape(16, 32, 256)
    piece = turn(order, piece)
    f = first_axis(piece, 1)
    g = first_axis(piece, -1)
    h = first_axis(f[:512], 1)
    i = first_axis(g[512:], -1)
    h0 = jnp.concatenate([piece, f], axis=1)
    h1 = jnp.concatenate([g, jnp.concatenate([h, i], axis=0)], axis=1)
    f0 = second_axis(h0, 1)
    g0 = second_axis(h0, -1)
    f1 = second_axis(h1, 1)
    g1 = second_axis(h1, -1)
    last0 = second_axis(f0, 1)
    last1 = second_axis(g1, -1)
    partial, ahead, so_far = tile_a(index, columns, [h0, h1, f0, f1, g0, g1], prior, spread)
    ahead, last0, last1 = lax.optimization_barrier((ahead, last0, last1))
    grm, rounded, image = tile_b(
        index, partial, ahead, last0, last1, spread, so_far, early[:, :1024]
    )
    gram1 = dot_t(image, image, ((1,), (1,)))
    packed = with_gram(dot_t(image.astype(BF16), rounded, ((1,), (1,))), gram1)
    packed = bcast_sum(packed, "x").astype(BF16)
    second, gram1 = split_gram(bcast_sum(packed, "y"))
    second, diagonal = solve(gram1, second)
    third, gram2 = row_sum(
        dot_t(second.astype(BF16), rounded, ((1,), (0,))), dot_t(second, second, ((1,), (1,)))
    )
    gram3 = jnp.pad(dot_t(third, third, ((1,), (1,))), ((0, 4), (0, 108)))
    gram3 = bcast_sum(gram3, COL)[:K, :K]
    vectors, spectrum = last(diagonal, gram2, gram3, third)
    return (grm, vectors.T, spectrum)


def solution(mesh):
    finer = Mesh(mesh.devices.reshape(SIZES), ALL)
    in_specs = (P(ALL, None), P(ALL), P(), P(ROW, COL), P(ROW, None))
    out_specs = (P(ROW, COL), P(COL, None), P())
    return jax.shard_map(body, mesh=finer, in_specs=in_specs, out_specs=out_specs, check_vma=False)
```

```python
import jax
import jax.numpy as jnp
from jax import lax
from jax.experimental import pallas as pl
from jax.experimental.pallas import tpu as pltpu
from jax.sharding import Mesh
from jax.sharding import PartitionSpec as P


S = 16384
M = 4096
K = 20
ROW = ("z", "core")
COL = ("x", "y")
ALL = ("z", "core", "x", "y")
SIZES = (8, 2, 4, 4)
F32 = jnp.float32
BF16 = jnp.bfloat16
VMEM = pl.BlockSpec(memory_space=pltpu.VMEM)
ANY = pl.BlockSpec(memory_space=pl.ANY)
SMEM = pl.BlockSpec(memory_space=pltpu.SMEM)


def place(z, core, x, y):
    return ((z * 2 + core) * 4 + x) * 4 + y


def send(array, target):
    pairs = []
    for z in range(8):
        for core in range(2):
            for x in range(4):
                for y in range(4):
                    pairs.append((place(z, core, x, y), place(*target(z, core, x, y))))
    return lax.ppermute(array, ALL, pairs)


def swap_core(array):
    return send(array, lambda z, core, x, y: (z, 1 - core, x, y))


def ring_z(array):
    return send(array, lambda z, core, x, y: ((z + 1 - 2 * core) % 8, core, x, y))


def first_axis(array, step):
    def target(z, core, x, y):
        return (z, core, (x + step) % 4, y) if core == 0 else (z, core, x, (y + step) % 4)

    return send(array, target)


def second_axis(array, step):
    def target(z, core, x, y):
        return (z, core, (x + step) % 4, y) if core == 1 else (z, core, x, (y + step) % 4)

    return send(array, target)


def standardize_kernel(index, table, genotypes, out, rows, doubled, spread):
    count = genotypes.shape[0]

    @pl.when(pl.program_id(0) == 0)
    def _():
        lane = lax.broadcasted_iota(jnp.int32, (count, 128), 1)
        sub = lax.broadcasted_iota(jnp.int32, (count, 128), 0)
        want = jnp.zeros((count, 128), jnp.int32)
        for j in range(count):
            rows[pl.ds(j, 1), :] = table[pl.ds(index[j] // 128, 1), :]
            want = jnp.where(sub == j, index[j] % 128, want)
        freq = jnp.sum(jnp.where(lane == want, rows[...], 0.0), axis=1, keepdims=True)
        doubled[...] = jnp.broadcast_to(2.0 * freq, (count, 128))
        spread[...] = jnp.broadcast_to(jnp.sqrt(2.0 * freq * (1.0 - freq)), (count, 128))

    blocks = out.shape[0]
    for i in range(blocks):
        value = genotypes[:, 1024 * i : 1024 * (i + 1)].astype(F32) - doubled[:, :1]
        out[i] = (value / spread[:, :1]).astype(BF16)


def standardize(genotypes, snp_index, freq_table):
    snps, _ = genotypes.shape
    return pl.pallas_call(
        standardize_kernel,
        grid_spec=pltpu.PrefetchScalarGridSpec(
            num_scalar_prefetch=1,
            grid=(4,),
            in_specs=[
                pl.BlockSpec((128, 128), lambda i, s: (0, 0)),
                pl.BlockSpec((snps, 4096), lambda i, s: (0, i)),
            ],
            out_specs=pl.BlockSpec((4, snps, 1024), lambda i, s: (i, 0, 0)),
            scratch_shapes=[pltpu.VMEM((snps, 128), F32)] * 3,
        ),
        out_shape=jax.ShapeDtypeStruct((16, snps, 1024), BF16),
        compiler_params=pltpu.CompilerParams(vmem_limit_bytes=60 * 2**20),
        name="standardize",
    )(snp_index, freq_table.reshape(128, 128), genotypes)


def turn_kernel(order, piece, out, stage):
    for j in range(16):
        stage[16 * j : 16 * (j + 1), :] = piece[order[j]]
    out[...] = stage[...].T


def turn(order, piece):
    return pl.pallas_call(
        turn_kernel,
        in_specs=[SMEM, VMEM],
        out_specs=VMEM,
        out_shape=jax.ShapeDtypeStruct((1024, 256), BF16),
        scratch_shapes=[pltpu.VMEM((256, 1024), BF16)],
        compiler_params=pltpu.CompilerParams(vmem_limit_bytes=8 * 2**20),
        name="turn",
    )(order, piece)


def fetch_columns(index, columns, target, sem, first):
    for t in range(2):
        which = index[first + t]
        for j in range(16):
            pltpu.make_async_copy(
                columns[j].at[which], target.at[pl.ds(256 * t + 16 * j, 16)], sem
            ).start()


def tile_kernel(index, *refs):
    columns, rows = refs[:16], refs[16:24]
    prior, spread, first = refs[24:27]
    out, rounded, image = refs[27:30]
    total, old, left, stage, old_sem, left_sem, stage_sem, out_sem = refs[30:]

    def fetch_row(i):
        return pltpu.make_async_copy(rows[i], left.at[i, pl.ds(0, 1024)], left_sem.at[i])

    fetch_old = pltpu.make_async_copy(prior, old, old_sem)
    for i in range(8):
        fetch_row(i).start()
        fetch_columns(index, columns, stage.at[i], stage_sem.at[i], 2 * i)
        if i == 5:
            fetch_old.start()
    for i in range(8):
        for t in range(2):
            left[i, 1024:1056, 256 * t : 256 * (t + 1)] = spread[index[2 * i + t]]
    for group in range(4):
        for i in (2 * group, 2 * group + 1):
            fetch_row(i).wait()
            pltpu.make_async_copy(stage.at[i], stage.at[i], stage_sem.at[i]).wait()
        if group == 3:
            fetch_old.wait()

        def step(n, carry, group=group):
            at = pl.ds(pl.multiple_of(n * 256, 256), 256)
            product = jnp.zeros((1056, 256), F32)
            for i in (2 * group, 2 * group + 1):
                product += jnp.dot(left[i], stage[i, :, at], preferred_element_type=F32)
            if group == 0:
                total[:, at] = product
            elif group < 3:
                total[:, at] += product
            else:
                product += total[:, at]
                value = old[:, at] + product[:1024] * (1.0 / M)
                old[:, at] = value
                pltpu.make_async_copy(old.at[:, at], out.at[:, at], out_sem.at[n]).start()
                rounded[:, at] = value.astype(BF16)
                image[:, at] = first[:, at] + product[1024 : 1024 + K] * (1.0 / M)
            return carry

        lax.fori_loop(0, 4, step, 0)
    for n in range(4):
        at = pl.ds(n * 256, 256)
        pltpu.make_async_copy(old.at[:, at], out.at[:, at], out_sem.at[n]).wait()


def tile(index, columns, rows, prior, spread, first):
    return pl.pallas_call(
        tile_kernel,
        in_specs=[SMEM] + [ANY] * 25 + [VMEM] * 2,
        out_specs=[ANY, VMEM, VMEM],
        out_shape=[
            jax.ShapeDtypeStruct((1024, 1024), F32),
            jax.ShapeDtypeStruct((1024, 1024), BF16),
            jax.ShapeDtypeStruct((K, 1024), F32),
        ],
        scratch_shapes=[
            pltpu.VMEM((1056, 1024), F32),
            pltpu.VMEM((1024, 1024), F32),
            pltpu.VMEM((8, 1056, 512), BF16),
            pltpu.VMEM((8, 512, 1024), BF16),
            pltpu.SemaphoreType.DMA,
            pltpu.SemaphoreType.DMA((8,)),
            pltpu.SemaphoreType.DMA((8,)),
            pltpu.SemaphoreType.DMA((4,)),
        ],
        compiler_params=pltpu.CompilerParams(vmem_limit_bytes=40 * 2**20),
        cost_estimate=pl.CostEstimate(flops=8 * 2**30, bytes_accessed=26 * 2**20, transcendentals=0),
        name="tile",
    )(index, *columns, *rows, prior, spread, first)


def bcast_sum(array, axis):
    length = lax.axis_size(axis)
    copies = jnp.broadcast_to(array[None], (length, *array.shape))
    return lax.all_to_all(copies, axis, 0, 0, tiled=True).astype(F32).sum(axis=0)


def with_gram(wide, gram):
    width, quarter = wide.shape[1], K * K // 4
    high = lax.reduce_precision(gram, 8, 7)
    flat = jnp.concatenate([high.reshape(4, quarter), (gram - high).reshape(4, quarter)], axis=1)
    flat = jnp.pad(flat, ((0, 0), (0, width - 2 * quarter)))
    return jnp.concatenate([wide, flat], axis=0).astype(BF16)


def split_gram(packed):
    quarter = K * K // 4
    flat = packed[K:, :quarter] + packed[K:, quarter : 2 * quarter]
    return packed[:K], flat.reshape(K, K)


def row_sum(wide, gram=None):
    half = wide.shape[1] // 2
    first = lax.axis_index("core") == 0
    lo, hi = wide[:, :half], wide[:, half:]
    keep, give = jnp.where(first, lo, hi), jnp.where(first, hi, lo)
    mine = keep + swap_core(give)
    if gram is None:
        mine = bcast_sum(mine.astype(BF16), "z")
    else:
        mine, gram = split_gram(bcast_sum(with_gram(mine, gram), "z"))
        gram = gram + swap_core(gram)
    other = swap_core(mine)
    full = jnp.where(
        first,
        jnp.concatenate([mine, other], axis=1),
        jnp.concatenate([other, mine], axis=1),
    )
    return full if gram is None else (full, gram)


def dot_t(a, b, dims):
    return lax.dot_general(a, b, (dims, ((), ())), preferred_element_type=F32)


def eliminate(gram, wide=None):
    row = lax.broadcasted_iota(jnp.int32, (K, 1), 0)
    for j in range(K - 1):
        factor = jnp.where(row > j, gram[:, j : j + 1] / gram[j : j + 1, j : j + 1], 0.0)
        if wide is not None:
            wide = wide - factor * wide[j : j + 1, :]
        gram = gram - factor * gram[j : j + 1, :]
    eye = row == lax.broadcasted_iota(jnp.int32, (K, K), 1)
    pivots = jnp.where(eye, gram, 0.0)
    if wide is not None:
        wide = wide / jnp.sqrt(jnp.sum(pivots, axis=1, keepdims=True))
    return jnp.sqrt(jnp.sum(pivots, axis=0, keepdims=True)), wide


def solve_kernel(gram, wide, out, diagonal):
    diagonal[...], out[...] = eliminate(gram[...], wide[...])


def solve(gram, wide):
    return pl.pallas_call(
        solve_kernel,
        in_specs=[VMEM] * 2,
        out_specs=[VMEM] * 2,
        out_shape=[jax.ShapeDtypeStruct(wide.shape, F32), jax.ShapeDtypeStruct((1, K), F32)],
        compiler_params=pltpu.CompilerParams(vmem_limit_bytes=4 * 2**20),
        name="solve",
    )(gram, wide)


def last_kernel(first, gram2, gram3, wide, out, spectrum):
    second, _ = eliminate(gram2[...])
    third, vectors = eliminate(gram3[...], wide[...])
    out[...] = vectors * jnp.sqrt(F32(S))
    spectrum[0:1, :] = first[...]
    spectrum[1:2, :] = second
    spectrum[2:3, :] = third / second


def last(first, gram2, gram3, wide):
    return pl.pallas_call(
        last_kernel,
        in_specs=[VMEM] * 4,
        out_specs=[VMEM] * 2,
        out_shape=[jax.ShapeDtypeStruct(wide.shape, F32), jax.ShapeDtypeStruct((3, K), F32)],
        compiler_params=pltpu.CompilerParams(vmem_limit_bytes=4 * 2**20),
        name="last",
    )(first, gram2, gram3, wide)


def body(genotypes, snp_index, freq_table, prior, start_vectors):
    z, core, x, y = (lax.axis_index(a) for a in ALL)
    sign = 1 - 2 * core
    steps = jnp.array([0, 0, -1, -1, -2, -2, -3, -3, -4, 1, 1, 2, 2, 3, 3, 4], jnp.int32)
    flips = jnp.array([0, 1, 0, 1, 0, 1, 0, 1, 0, 1, 0, 1, 0, 1, 0, 1], jnp.int32)
    order = ((z + sign * steps) % 8) * 2 + (core + flips) % 2
    along = jnp.array([0, -1, 1, 2] * 4, jnp.int32)
    across = jnp.array([0] * 4 + [-1] * 4 + [1] * 4 + [2] * 4, jnp.int32)
    index = ((x + jnp.where(core == 0, along, across)) % 4) * 4 + (
        y + jnp.where(core == 0, across, along)
    ) % 4

    standard = standardize(genotypes, snp_index, freq_table)
    piece = lax.all_to_all(standard, ROW, 0, 0, tiled=True)
    standard, piece = lax.optimization_barrier((standard, piece))
    own = lax.all_to_all(standard, COL, 0, 0, tiled=True)
    a, b = own, swap_core(own)
    down, up = [a, b], []
    for j in range(1, 5):
        a = ring_z(a)
        down.append(a)
        up.append(swap_core(a))
        if j < 4:
            b = ring_z(b)
            down.append(b)
            up.append(swap_core(b))
    columns = down + up

    start = (start_vectors.T / jnp.sqrt(F32(S))).astype(BF16)
    of_prior = dot_t(start, prior.astype(BF16), ((1,), (0,)))
    of_piece = dot_t(start, piece.reshape(256, 1024), ((1,), (1,)))
    early = row_sum(jnp.concatenate([of_prior, of_piece], axis=1))
    spread = jnp.pad(early[:, 1024:], ((0, 32 - K), (0, 0))).astype(BF16)
    spread = lax.all_to_all(jnp.broadcast_to(spread[None], (16, 32, 256)), COL, 0, 0, tiled=True)
    at = jnp.arange(256, dtype=jnp.int32)
    moved = jnp.broadcast_to(order[:, None], (16, 16)).reshape(1, 256) * 16 + at[None] % 16
    moved = (at[:, None] == moved).astype(BF16)
    spread = dot_t(spread.reshape(512, 256), moved, ((1,), (0,))).astype(BF16)
    spread = spread.reshape(16, 32, 256)
    piece = turn(order, piece)
    f = first_axis(piece, 1)
    g = first_axis(piece, -1)
    h = first_axis(f[:512], 1)
    i = first_axis(g[512:], -1)
    h0 = jnp.concatenate([piece, f], axis=1)
    h1 = jnp.concatenate([g, jnp.concatenate([h, i], axis=0)], axis=1)
    f0 = second_axis(h0, 1)
    g0 = second_axis(h0, -1)
    f1 = second_axis(h1, 1)
    g1 = second_axis(h1, -1)
    last0 = second_axis(f0, 1)
    last1 = second_axis(g1, -1)
    rows = [h0, h1, f0, f1, g0, g1, last0, last1]
    grm, rounded, image = tile(index, columns, rows, prior, spread, early[:, :1024])
    gram1 = dot_t(image, image, ((1,), (1,)))
    packed = with_gram(dot_t(image.astype(BF16), rounded, ((1,), (1,))), gram1)
    packed = bcast_sum(packed, "x").astype(BF16)
    second, gram1 = split_gram(bcast_sum(packed, "y"))
    second, diagonal = solve(gram1, second)
    third, gram2 = row_sum(
        dot_t(second.astype(BF16), rounded, ((1,), (0,))), dot_t(second, second, ((1,), (1,)))
    )
    gram3 = jnp.pad(dot_t(third, third, ((1,), (1,))), ((0, 4), (0, 108)))
    gram3 = bcast_sum(gram3, COL)[:K, :K]
    vectors, spectrum = last(diagonal, gram2, gram3, third)
    return (grm, vectors.T, spectrum)


def solution(mesh):
    finer = Mesh(mesh.devices.reshape(SIZES), ALL)
    in_specs = (P(ALL, None), P(ALL), P(), P(ROW, COL), P(ROW, None))
    out_specs = (P(ROW, COL), P(COL, None), P())
    return jax.shard_map(body, mesh=finer, in_specs=in_specs, out_specs=out_specs, check_vma=False)
```

```python
import jax
import jax.numpy as jnp
from jax import lax
from jax.experimental import pallas as pl
from jax.experimental.pallas import tpu as pltpu
from jax.sharding import Mesh
from jax.sharding import PartitionSpec as P


S = 16384
M = 4096
K = 20
ROW = ("z", "core")
COL = ("x", "y")
ALL = ("z", "core", "x", "y")
SIZES = (8, 2, 4, 4)
F32 = jnp.float32
BF16 = jnp.bfloat16
VMEM = pl.BlockSpec(memory_space=pltpu.VMEM)
ANY = pl.BlockSpec(memory_space=pl.ANY)
SMEM = pl.BlockSpec(memory_space=pltpu.SMEM)


def place(z, core, x, y):
    return ((z * 2 + core) * 4 + x) * 4 + y


def send(array, target):
    pairs = []
    for z in range(8):
        for core in range(2):
            for x in range(4):
                for y in range(4):
                    pairs.append((place(z, core, x, y), place(*target(z, core, x, y))))
    return lax.ppermute(array, ALL, pairs)


def swap_core(array):
    return send(array, lambda z, core, x, y: (z, 1 - core, x, y))


def ring_z(array):
    return send(array, lambda z, core, x, y: ((z + 1 - 2 * core) % 8, core, x, y))


def first_axis(array, step):
    def target(z, core, x, y):
        return (z, core, (x + step) % 4, y) if core == 0 else (z, core, x, (y + step) % 4)

    return send(array, target)


def second_axis(array, step):
    def target(z, core, x, y):
        return (z, core, (x + step) % 4, y) if core == 1 else (z, core, x, (y + step) % 4)

    return send(array, target)


def standardize_kernel(index, table, genotypes, out, rows, doubled, spread):
    count = genotypes.shape[0]

    @pl.when(pl.program_id(0) == 0)
    def _():
        lane = lax.broadcasted_iota(jnp.int32, (count, 128), 1)
        sub = lax.broadcasted_iota(jnp.int32, (count, 128), 0)
        want = jnp.zeros((count, 128), jnp.int32)
        for j in range(count):
            rows[pl.ds(j, 1), :] = table[pl.ds(index[j] // 128, 1), :]
            want = jnp.where(sub == j, index[j] % 128, want)
        freq = jnp.sum(jnp.where(lane == want, rows[...], 0.0), axis=1, keepdims=True)
        doubled[...] = jnp.broadcast_to(2.0 * freq, (count, 128))
        spread[...] = jnp.broadcast_to(jnp.sqrt(2.0 * freq * (1.0 - freq)), (count, 128))

    blocks = out.shape[0]
    for i in range(blocks):
        value = genotypes[:, 1024 * i : 1024 * (i + 1)].astype(F32) - doubled[:, :1]
        out[i] = (value / spread[:, :1]).astype(BF16)


def standardize(genotypes, snp_index, freq_table):
    snps, _ = genotypes.shape
    return pl.pallas_call(
        standardize_kernel,
        grid_spec=pltpu.PrefetchScalarGridSpec(
            num_scalar_prefetch=1,
            grid=(4,),
            in_specs=[
                pl.BlockSpec((128, 128), lambda i, s: (0, 0)),
                pl.BlockSpec((snps, 4096), lambda i, s: (0, i)),
            ],
            out_specs=pl.BlockSpec((4, snps, 1024), lambda i, s: (i, 0, 0)),
            scratch_shapes=[pltpu.VMEM((snps, 128), F32)] * 3,
        ),
        out_shape=jax.ShapeDtypeStruct((16, snps, 1024), BF16),
        compiler_params=pltpu.CompilerParams(vmem_limit_bytes=60 * 2**20),
        name="standardize",
    )(snp_index, freq_table.reshape(128, 128), genotypes)


def turn_kernel(order, piece, out, stage):
    for j in range(16):
        stage[16 * j : 16 * (j + 1), :] = piece[order[j]]
    out[...] = stage[...].T


def turn(order, piece):
    return pl.pallas_call(
        turn_kernel,
        in_specs=[SMEM, VMEM],
        out_specs=VMEM,
        out_shape=jax.ShapeDtypeStruct((1024, 256), BF16),
        scratch_shapes=[pltpu.VMEM((256, 1024), BF16)],
        compiler_params=pltpu.CompilerParams(vmem_limit_bytes=8 * 2**20),
        name="turn",
    )(order, piece)


def fetch_columns(index, columns, target, sem, first):
    for t in range(2):
        which = index[first + t]
        for j in range(16):
            pltpu.make_async_copy(
                columns[j].at[which], target.at[pl.ds(256 * t + 16 * j, 16)], sem
            ).start()


def tile_kernel(index, *refs):
    columns, rows = refs[:16], refs[16:24]
    prior, spread, first = refs[24:27]
    out, rounded, second, gram = refs[27:31]
    total, old, image, left, stage, old_sem, left_sem, stage_sem, out_sem = refs[31:]

    def fetch_row(i):
        return pltpu.make_async_copy(rows[i], left.at[i, pl.ds(0, 1024)], left_sem.at[i])

    fetch_old = pltpu.make_async_copy(prior, old, old_sem)
    for i in range(8):
        fetch_row(i).start()
        fetch_columns(index, columns, stage.at[i], stage_sem.at[i], 2 * i)
        if i == 5:
            fetch_old.start()
    for i in range(8):
        for t in range(2):
            left[i, 1024:1056, 256 * t : 256 * (t + 1)] = spread[index[2 * i + t]]
    for group in range(4):
        for i in (2 * group, 2 * group + 1):
            fetch_row(i).wait()
            pltpu.make_async_copy(stage.at[i], stage.at[i], stage_sem.at[i]).wait()
        if group == 3:
            fetch_old.wait()

        def step(n, carry, group=group):
            at = pl.ds(pl.multiple_of(n * 256, 256), 256)
            product = jnp.zeros((1056, 256), F32)
            for i in (2 * group, 2 * group + 1):
                product += jnp.dot(left[i], stage[i, :, at], preferred_element_type=F32)
            if group == 0:
                total[:, at] = product
            elif group < 3:
                total[:, at] += product
            else:
                product += total[:, at]
                value = old[:, at] + product[:1024] * (1.0 / M)
                old[:, at] = value
                pltpu.make_async_copy(old.at[:, at], out.at[:, at], out_sem.at[n]).start()
                rounded[:, at] = value.astype(BF16)
                image[:, at] = first[:, at] + product[1024 : 1024 + K] * (1.0 / M)
            return carry

        lax.fori_loop(0, 4, step, 0)
    vectors = image[...]
    second[...] = dot_t(vectors.astype(BF16), rounded[...], ((1,), (1,)))
    gram[...] = dot_t(vectors, vectors, ((1,), (1,)))
    for n in range(4):
        at = pl.ds(n * 256, 256)
        pltpu.make_async_copy(old.at[:, at], out.at[:, at], out_sem.at[n]).wait()


def tile(index, columns, rows, prior, spread, first):
    return pl.pallas_call(
        tile_kernel,
        in_specs=[SMEM] + [ANY] * 25 + [VMEM] * 2,
        out_specs=[ANY, VMEM, VMEM, VMEM],
        out_shape=[
            jax.ShapeDtypeStruct((1024, 1024), F32),
            jax.ShapeDtypeStruct((1024, 1024), BF16),
            jax.ShapeDtypeStruct((K, 1024), F32),
            jax.ShapeDtypeStruct((K, K), F32),
        ],
        scratch_shapes=[
            pltpu.VMEM((1056, 1024), F32),
            pltpu.VMEM((1024, 1024), F32),
            pltpu.VMEM((K, 1024), F32),
            pltpu.VMEM((8, 1056, 512), BF16),
            pltpu.VMEM((8, 512, 1024), BF16),
            pltpu.SemaphoreType.DMA,
            pltpu.SemaphoreType.DMA((8,)),
            pltpu.SemaphoreType.DMA((8,)),
            pltpu.SemaphoreType.DMA((4,)),
        ],
        compiler_params=pltpu.CompilerParams(vmem_limit_bytes=40 * 2**20),
        cost_estimate=pl.CostEstimate(flops=8 * 2**30, bytes_accessed=26 * 2**20, transcendentals=0),
        name="tile",
    )(index, *columns, *rows, prior, spread, first)


def bcast_sum(array, axis):
    length = lax.axis_size(axis)
    copies = jnp.broadcast_to(array[None], (length, *array.shape))
    return lax.all_to_all(copies, axis, 0, 0, tiled=True).astype(F32).sum(axis=0)


def with_gram(wide, gram):
    width, quarter = wide.shape[1], K * K // 4
    high = lax.reduce_precision(gram, 8, 7)
    flat = jnp.concatenate([high.reshape(4, quarter), (gram - high).reshape(4, quarter)], axis=1)
    flat = jnp.pad(flat, ((0, 0), (0, width - 2 * quarter)))
    return jnp.concatenate([wide, flat], axis=0).astype(BF16)


def split_gram(packed):
    quarter = K * K // 4
    flat = packed[K:, :quarter] + packed[K:, quarter : 2 * quarter]
    return packed[:K], flat.reshape(K, K)


def row_sum(wide, gram=None):
    half = wide.shape[1] // 2
    first = lax.axis_index("core") == 0
    lo, hi = wide[:, :half], wide[:, half:]
    keep, give = jnp.where(first, lo, hi), jnp.where(first, hi, lo)
    mine = keep + swap_core(give)
    if gram is None:
        mine = bcast_sum(mine.astype(BF16), "z")
    else:
        mine, gram = split_gram(bcast_sum(with_gram(mine, gram), "z"))
        gram = gram + swap_core(gram)
    other = swap_core(mine)
    full = jnp.where(
        first,
        jnp.concatenate([mine, other], axis=1),
        jnp.concatenate([other, mine], axis=1),
    )
    return full if gram is None else (full, gram)


def dot_t(a, b, dims):
    return lax.dot_general(a, b, (dims, ((), ())), preferred_element_type=F32)


def eliminate(gram, wide=None):
    row = lax.broadcasted_iota(jnp.int32, (K, 1), 0)
    for j in range(K - 1):
        factor = jnp.where(row > j, gram[:, j : j + 1] / gram[j : j + 1, j : j + 1], 0.0)
        if wide is not None:
            wide = wide - factor * wide[j : j + 1, :]
        gram = gram - factor * gram[j : j + 1, :]
    eye = row == lax.broadcasted_iota(jnp.int32, (K, K), 1)
    pivots = jnp.where(eye, gram, 0.0)
    if wide is not None:
        wide = wide / jnp.sqrt(jnp.sum(pivots, axis=1, keepdims=True))
    return jnp.sqrt(jnp.sum(pivots, axis=0, keepdims=True)), wide


def solve_kernel(gram, wide, out, diagonal):
    diagonal[...], out[...] = eliminate(gram[...], wide[...])


def solve(gram, wide):
    return pl.pallas_call(
        solve_kernel,
        in_specs=[VMEM] * 2,
        out_specs=[VMEM] * 2,
        out_shape=[jax.ShapeDtypeStruct(wide.shape, F32), jax.ShapeDtypeStruct((1, K), F32)],
        compiler_params=pltpu.CompilerParams(vmem_limit_bytes=4 * 2**20),
        name="solve",
    )(gram, wide)


def last_kernel(first, gram2, gram3, wide, out, spectrum):
    second, _ = eliminate(gram2[...])
    third, vectors = eliminate(gram3[...], wide[...])
    out[...] = vectors * jnp.sqrt(F32(S))
    spectrum[0:1, :] = first[...]
    spectrum[1:2, :] = second
    spectrum[2:3, :] = third / second


def last(first, gram2, gram3, wide):
    return pl.pallas_call(
        last_kernel,
        in_specs=[VMEM] * 4,
        out_specs=[VMEM] * 2,
        out_shape=[jax.ShapeDtypeStruct(wide.shape, F32), jax.ShapeDtypeStruct((3, K), F32)],
        compiler_params=pltpu.CompilerParams(vmem_limit_bytes=4 * 2**20),
        name="last",
    )(first, gram2, gram3, wide)


def body(genotypes, snp_index, freq_table, prior, start_vectors):
    z, core, x, y = (lax.axis_index(a) for a in ALL)
    sign = 1 - 2 * core
    steps = jnp.array([0, 0, -1, -1, -2, -2, -3, -3, -4, 1, 1, 2, 2, 3, 3, 4], jnp.int32)
    flips = jnp.array([0, 1, 0, 1, 0, 1, 0, 1, 0, 1, 0, 1, 0, 1, 0, 1], jnp.int32)
    order = ((z + sign * steps) % 8) * 2 + (core + flips) % 2
    along = jnp.array([0, -1, 1, 2] * 4, jnp.int32)
    across = jnp.array([0] * 4 + [-1] * 4 + [1] * 4 + [2] * 4, jnp.int32)
    index = ((x + jnp.where(core == 0, along, across)) % 4) * 4 + (
        y + jnp.where(core == 0, across, along)
    ) % 4

    standard = standardize(genotypes, snp_index, freq_table)
    piece = lax.all_to_all(standard, ROW, 0, 0, tiled=True)
    standard, piece = lax.optimization_barrier((standard, piece))
    own = lax.all_to_all(standard, COL, 0, 0, tiled=True)
    a, b = own, swap_core(own)
    down, up = [a, b], []
    for j in range(1, 5):
        a = ring_z(a)
        down.append(a)
        up.append(swap_core(a))
        if j < 4:
            b = ring_z(b)
            down.append(b)
            up.append(swap_core(b))
    columns = down + up

    start = (start_vectors.T / jnp.sqrt(F32(S))).astype(BF16)
    of_prior = dot_t(start, prior.astype(BF16), ((1,), (0,)))
    of_piece = dot_t(start, piece.reshape(256, 1024), ((1,), (1,)))
    early = row_sum(jnp.concatenate([of_prior, of_piece], axis=1))
    spread = jnp.pad(early[:, 1024:], ((0, 32 - K), (0, 0))).astype(BF16)
    spread = lax.all_to_all(jnp.broadcast_to(spread[None], (16, 32, 256)), COL, 0, 0, tiled=True)
    at = jnp.arange(256, dtype=jnp.int32)
    moved = jnp.broadcast_to(order[:, None], (16, 16)).reshape(1, 256) * 16 + at[None] % 16
    moved = (at[:, None] == moved).astype(BF16)
    spread = dot_t(spread.reshape(512, 256), moved, ((1,), (0,))).astype(BF16)
    spread = spread.reshape(16, 32, 256)
    piece = turn(order, piece)
    f = first_axis(piece, 1)
    g = first_axis(piece, -1)
    h = first_axis(f[:512], 1)
    i = first_axis(g[512:], -1)
    h0 = jnp.concatenate([piece, f], axis=1)
    h1 = jnp.concatenate([g, jnp.concatenate([h, i], axis=0)], axis=1)
    f0 = second_axis(h0, 1)
    g0 = second_axis(h0, -1)
    f1 = second_axis(h1, 1)
    g1 = second_axis(h1, -1)
    last0 = second_axis(f0, 1)
    last1 = second_axis(g1, -1)
    rows = [h0, h1, f0, f1, g0, g1, last0, last1]
    grm, rounded, second, gram1 = tile(index, columns, rows, prior, spread, early[:, :1024])
    packed = with_gram(second, gram1)
    packed = bcast_sum(packed, "x").astype(BF16)
    second, gram1 = split_gram(bcast_sum(packed, "y"))
    second, diagonal = solve(gram1, second)
    third, gram2 = row_sum(
        dot_t(second.astype(BF16), rounded, ((1,), (0,))), dot_t(second, second, ((1,), (1,)))
    )
    gram3 = jnp.pad(dot_t(third, third, ((1,), (1,))), ((0, 4), (0, 108)))
    gram3 = bcast_sum(gram3, COL)[:K, :K]
    vectors, spectrum = last(diagonal, gram2, gram3, third)
    return (grm, vectors.T, spectrum)


def solution(mesh):
    finer = Mesh(mesh.devices.reshape(SIZES), ALL)
    in_specs = (P(ALL, None), P(ALL), P(), P(ROW, COL), P(ROW, None))
    out_specs = (P(ROW, COL), P(COL, None), P())
    return jax.shard_map(body, mesh=finer, in_specs=in_specs, out_specs=out_specs, check_vma=False)
```
